32 devices in a mesh: gz: 4 (over z), gx: 4 (over y, x), gy: 2 (over core).
Axes of the slice: x: 2, y: 2, z: 4, core: 2. Of those that a mesh axis runs over, the one named last changes fastest.
Arguments:
- density: float32 [128, 256, 1024], P('gz', 'gy', 'gx'), may hold values from 0 to 1
- mask: int32 [16, 32, 128], P('gz', 'gy', 'gx'), may hold values from 0 to 3
Outputs:
- filtered: float32 [128, 256, 1024], P(('gz', 'gx'), 'gy')
- projected: float32 [128, 256, 1024], P(('gz', 'gx'), 'gy')
The draws below stay inside these ranges and needn't reach their ends.
Inputs may be any that keep to these rules, and one draw needn't show every extreme that they name: `mask`: code 0 marks a void block, 1 a solid block, 2 and 3 design blocks.
All inputs are finite; a program needn't handle non-finite values.
Results may differ from the reference program's by a relative error of at most 0.0003.
Values sent between devices are 32-bit elements; how exact they have to be, the bound alone decides.
A program may use at most 128 MiB of HBM per device.

```python
import jax
import jax.numpy as jnp
from jax import lax

RADIUS = 6
CELLS = 8
NX = 1024
NY = 256
NZ = 128


def set_ends(drawn, rng, smallest, high):
    dims = drawn.shape
    spot = [jax.random.randint(jax.random.fold_in(rng, axis), (), 0, dims[axis]) for axis in range(len(dims))]
    drawn = drawn.at[tuple(spot)].set(smallest)
    longest = dims.index(max(dims))
    spot[longest] = (spot[longest] + 1) % dims[longest]
    return drawn.at[tuple(spot)].set(high)


def steps_of(stream_key, shape, split, low, high):
    level = 1.0
    for dim, parts in split:
        steps = jax.random.uniform(jax.random.fold_in(jax.random.fold_in(stream_key, 6), dim), (parts,), jnp.float32, low / len(split), high / len(split))
        level = level * jnp.repeat(jnp.exp(steps), shape[dim] // parts).reshape((-1,) + (1,) * (len(shape) - 1 - dim))
    return level


def setup_inputs(seed: int = 0) -> dict:
    splits = jax.random.split(jax.random.key(seed), 3)
    return {
        "density": jnp.clip(1.0 * jax.random.uniform(splits[0], (NZ, NY, NX), jnp.float32) ** steps_of(splits[0], (NZ, NY, NX), ((0, 4), (1, 2), (2, 4)), -0.2, 0.2), 0.0, 1.0),
        "mask": set_ends(jax.random.randint(splits[1], (NZ // CELLS, NY // CELLS, NX // CELLS), 0, 4), jax.random.fold_in(splits[1], 1), 0, 3).astype(jnp.int32),
    }


sharpness = 8.0
threshold = 0.5


def smooth_axis(values, axis_index, count):
    widths = [(RADIUS, RADIUS) if position == axis_index else (0, 0) for position in range(values.ndim)]
    padded = jnp.pad(values, widths)
    result = jnp.zeros_like(values)
    for offset in range(-RADIUS, RADIUS + 1):
        window = lax.slice_in_dim(padded, RADIUS + offset, RADIUS + offset + count, axis=axis_index)
        result = result + float(RADIUS + 1 - abs(offset)) * window
    return result


def weight_count(count):
    return smooth_axis(jnp.ones((count,), jnp.float32), 0, count)


def reference(density, mask):
    def one_plane(item):
        plane, level = item
        block_row = mask[level // CELLS]
        design_code = jnp.repeat(jnp.repeat(block_row, CELLS, 0), CELLS, 1)
        physical = jnp.where(design_code == 0, 0.0, jnp.where(design_code == 1, 1.0, plane))
        return smooth_axis(smooth_axis(physical, 1, NX), 0, NY)

    levels = jnp.arange(NZ, dtype=jnp.int32)
    flat = lax.map(one_plane, (density, levels))
    summed = smooth_axis(flat, 0, NZ)
    counts = weight_count(NZ)[:, None, None] * weight_count(NY)[None, :, None] * weight_count(NX)[None, None, :]
    filtered = summed / counts
    top = jnp.tanh(sharpness * threshold)
    projected = (top + jnp.tanh(sharpness * (filtered - threshold))) / (top + jnp.tanh(sharpness * (1.0 - threshold)))
    return filtered, projected
```

```python
import functools
import math

import jax
import jax.numpy as jnp
from jax import lax
from jax.experimental import pallas as pl
from jax.experimental.pallas import tpu as pltpu
from jax.sharding import PartitionSpec as P

RADIUS = 6
CELLS = 8
LANES = 128
SUBLANES = 8

sharpness = 8.0
threshold = 0.5
MESH = pl.DeviceIdType.MESH


def hat(rows, cols, offset):
    row = lax.broadcasted_iota(jnp.int32, (rows, cols), 0)
    col = lax.broadcasted_iota(jnp.int32, (rows, cols), 1)
    return jnp.maximum(RADIUS + 1 - jnp.abs(col + offset - row), 0).astype(jnp.float32)


def halves(values):
    high = values.astype(jnp.bfloat16)
    low = (values - high.astype(jnp.float32)).astype(jnp.bfloat16)
    return high, low


def dot(a, b):
    return jnp.dot(a, b, preferred_element_type=jnp.float32)


def kernel(
    sizes,
    density,
    mask,
    out,
    phys,
    codes,
    masks,
    zf,
    recv,
    yb,
    xs,
    stage,
    w_own,
    w_edge,
    load_sem,
    mask_sem,
    hmask_send,
    hmask_recv,
    halo_send,
    halo_recv,
    send_sem,
    recv_sem,
    y_send,
    y_recv,
    out_sem,
):
    nz, nx, ny = sizes
    planes, rows, columns = density.shape
    blocks = mask.shape[0]
    layers = planes // nx
    gz, gx, gy = lax.axis_index("gz"), lax.axis_index("gx"), lax.axis_index("gy")
    has_up, has_down = gz > 0, gz < nz - 1
    has_prev, has_next = gy > 0, gy < ny - 1

    def load(b):
        part = pl.ds(b * CELLS, CELLS)
        return pltpu.make_async_copy(
            density.at[part], phys.at[pl.ds(RADIUS + b * CELLS, CELLS)], load_sem.at[b]
        )

    mask_copy = pltpu.make_async_copy(mask, masks.at[pl.ds(1, blocks)], mask_sem)
    mask_copy.start()
    for b in range(blocks):
        load(b).start()

    barrier = pltpu.get_barrier_semaphore()

    def greet(**where):
        pl.semaphore_signal(barrier, inc=1, device_id=where, device_id_type=MESH)

    pl.when(has_up)(lambda: greet(gz=gz - 1))
    pl.when(has_down)(lambda: greet(gz=gz + 1))
    pl.when(has_prev)(lambda: greet(gy=gy - 1))
    pl.when(has_next)(lambda: greet(gy=gy + 1))
    for step in range(1, nx):
        greet(gx=lax.rem(gx + step, nx))

    w_own[...] = hat(columns, columns, 0).astype(jnp.bfloat16)
    w_edge[pl.ds(0, LANES)] = hat(LANES, columns, LANES).astype(jnp.bfloat16)
    w_edge[pl.ds(LANES, LANES)] = hat(LANES, columns, -columns).astype(jnp.bfloat16)
    count = (
        nx
        - 1
        + has_up.astype(jnp.int32)
        + has_down.astype(jnp.int32)
        + has_prev.astype(jnp.int32)
        + has_next.astype(jnp.int32)
    )
    pl.semaphore_wait(barrier, count)

    def to_next(j):
        return pltpu.make_async_remote_copy(
            src_ref=density.at[planes - 1 - j],
            dst_ref=phys.at[RADIUS - 1 - j],
            send_sem=halo_send.at[0, j],
            recv_sem=halo_recv.at[0, j],
            device_id={"gz": gz + 1},
            device_id_type=MESH,
        )

    def to_previous(j):
        return pltpu.make_async_remote_copy(
            src_ref=density.at[j],
            dst_ref=phys.at[RADIUS + planes + j],
            send_sem=halo_send.at[1, j],
            recv_sem=halo_recv.at[1, j],
            device_id={"gz": gz - 1},
            device_id_type=MESH,
        )

    def mask_next():
        return pltpu.make_async_remote_copy(
            src_ref=mask.at[blocks - 1],
            dst_ref=masks.at[0],
            send_sem=hmask_send.at[0],
            recv_sem=hmask_recv.at[0],
            device_id={"gz": gz + 1},
            device_id_type=MESH,
        )

    def mask_previous():
        return pltpu.make_async_remote_copy(
            src_ref=mask.at[0],
            dst_ref=masks.at[blocks + 1],
            send_sem=hmask_send.at[1],
            recv_sem=hmask_recv.at[1],
            device_id={"gz": gz - 1},
            device_id_type=MESH,
        )

    @pl.when(has_down)
    def _():
        mask_next().start()
        for j in range(RADIUS):
            to_next(j).start()

    @pl.when(has_up)
    def _():
        mask_previous().start()
        for j in range(RADIUS):
            to_previous(j).start()

    def spread(b):
        small = masks[b].astype(jnp.float32).astype(jnp.bfloat16)
        mrows, mcols = small.shape
        r = lax.broadcasted_iota(jnp.int32, (rows, mrows), 0) // CELLS
        m = lax.broadcasted_iota(jnp.int32, (rows, mrows), 1)
        tall = dot(jnp.where(r == m, 1.0, 0.0).astype(jnp.bfloat16), small)
        c = lax.broadcasted_iota(jnp.int32, (mcols, columns), 1) // CELLS
        n = lax.broadcasted_iota(jnp.int32, (mcols, columns), 0)
        wide = jnp.where(c == n, 1.0, 0.0).astype(jnp.bfloat16)
        codes[b] = dot(tall.astype(jnp.bfloat16), wide)

    def apply_mask(row, b):
        code = codes[b]
        phys[row] = jnp.where(code < 0.5, 0.0, jnp.where(code < 1.5, 1.0, phys[row]))

    mask_copy.wait()
    for b in range(blocks):
        spread(b + 1)
    for b in range(blocks):
        load(b).wait()

    def mask_own(i, carry):
        apply_mask(RADIUS + i, 1 + i // CELLS)
        return carry

    lax.fori_loop(0, planes, mask_own, 0)

    @pl.when(jnp.logical_not(has_up))
    def _():
        phys[pl.ds(0, RADIUS)] = jnp.zeros((RADIUS, rows, columns), jnp.float32)

    @pl.when(jnp.logical_not(has_down))
    def _():
        phys[pl.ds(RADIUS + planes, RADIUS)] = jnp.zeros((RADIUS, rows, columns), jnp.float32)

    @pl.when(jnp.logical_not(has_prev))
    def _():
        yb[:, :, pl.ds(0, SUBLANES)] = jnp.zeros((layers, nx, SUBLANES, columns), jnp.float32)

    @pl.when(jnp.logical_not(has_next))
    def _():
        yb[:, :, pl.ds(SUBLANES, SUBLANES)] = jnp.zeros((layers, nx, SUBLANES, columns), jnp.float32)

    def piece(k, p, row):
        return pltpu.make_async_remote_copy(
            src_ref=zf.at[row],
            dst_ref=recv.at[k, gx],
            send_sem=send_sem.at[k, p],
            recv_sem=recv_sem.at[k, gx],
            device_id={"gx": p},
            device_id_type=MESH,
        )

    def z_step(k, carry):
        for p in range(nx):
            row = layers - 1 - k if p == 0 else p * layers + k
            part = rows // 4
            for i in range(4):
                at = pl.ds(i * part, part)
                run = phys[row + RADIUS, at]
                total = run
                for d in range(1, RADIUS + 1):
                    run = run + (phys[row + RADIUS - d, at] + phys[row + RADIUS + d, at])
                    total = total + run if d < RADIUS else total + run
                zf[row, at] = total

            @pl.when(gx != p)
            def _():
                piece(k, p, row).start()

            @pl.when(gx == p)
            def _():
                pltpu.make_async_copy(zf.at[row], recv.at[k, gx], recv_sem.at[k, gx]).start()

        return carry

    free = layers - RADIUS
    lax.fori_loop(0, free, z_step, 0)

    @pl.when(has_up)
    def _():
        mask_previous().wait_send()
        pltpu.make_async_copy(mask.at[0], masks.at[0], hmask_recv.at[0]).wait()
        spread(0)

    @pl.when(has_down)
    def _():
        mask_next().wait_send()
        pltpu.make_async_copy(mask.at[0], masks.at[blocks + 1], hmask_recv.at[1]).wait()
        spread(blocks + 1)

    def halo_step(k, carry):
        j = k - free

        @pl.when(has_up)
        def _():
            row = RADIUS - 1 - j
            pltpu.make_async_copy(density.at[0], phys.at[row], halo_recv.at[0, j]).wait()
            apply_mask(row, 0)

        @pl.when(has_down)
        def _():
            row = RADIUS + planes + j
            pltpu.make_async_copy(density.at[0], phys.at[row], halo_recv.at[1, j]).wait()
            apply_mask(row, blocks + 1)

        return z_step(k, carry)

    lax.fori_loop(free, layers, halo_step, 0)

    def y_previous(k):
        return pltpu.make_async_remote_copy(
            src_ref=recv.at[k, :, pl.ds(0, SUBLANES)],
            dst_ref=yb.at[k, :, pl.ds(SUBLANES, SUBLANES)],
            send_sem=y_send.at[k, 0],
            recv_sem=y_recv.at[k, 1],
            device_id={"gy": gy - 1},
            device_id_type=MESH,
        )

    def y_next(k):
        return pltpu.make_async_remote_copy(
            src_ref=recv.at[k, :, pl.ds(rows - SUBLANES, SUBLANES)],
            dst_ref=yb.at[k, :, pl.ds(0, SUBLANES)],
            send_sem=y_send.at[k, 1],
            recv_sem=y_recv.at[k, 0],
            device_id={"gy": gy + 1},
            device_id_type=MESH,
        )

    def x_filter(chunks, put):
        high, low = zip(*[halves(chunk) for chunk in chunks])
        none = jnp.zeros((chunks[0].shape[0], LANES), jnp.bfloat16)
        for c in range(nx):
            total = dot(high[c], w_own[...]) + dot(low[c], w_own[...])
            for part in (high, low):
                left = part[c - 1][:, columns - LANES :] if c > 0 else none
                right = part[c + 1][:, :LANES] if c < nx - 1 else none
                total = total + dot(jnp.concatenate([left, right], 1), w_edge[...])
            put(c, total)

    y_own = hat(rows, rows, 0).astype(jnp.bfloat16)
    y_edge = jnp.concatenate(
        [hat(rows, SUBLANES, -SUBLANES), hat(rows, SUBLANES, rows)], 1
    ).astype(jnp.bfloat16)

    def finish(k):
        layer = jnp.where(gx == 0, layers - 1 - k, k)
        return pltpu.make_async_copy(stage.at[k], out.at[layer], out_sem.at[k])

    def take_step(k, carry):
        for c in range(nx):
            pltpu.make_async_copy(zf.at[0], recv.at[k, c], recv_sem.at[k, c]).wait()
        pl.when(has_prev)(lambda: y_previous(k).start())
        pl.when(has_next)(lambda: y_next(k).start())

        def put_own(c, total):
            high, low = halves(total)
            at = pl.ds(c * columns, columns)
            xs[pl.ds(0, rows), at] = high
            xs[pl.ds(rows, rows), at] = low

        def put_edge(c, total):
            high, low = halves(total)
            at = pl.ds(c * columns, columns)
            xs[pl.ds(2 * rows, 2 * SUBLANES), at] = high
            xs[pl.ds(2 * rows + 2 * SUBLANES, 2 * SUBLANES), at] = low

        x_filter([recv[k, c] for c in range(nx)], put_own)

        @pl.when(has_prev)
        def _():
            y_previous(k).wait_send()
            part = yb.at[k, :, pl.ds(0, SUBLANES)]
            pltpu.make_async_copy(part, part, y_recv.at[k, 0]).wait()

        @pl.when(has_next)
        def _():
            y_next(k).wait_send()
            part = yb.at[k, :, pl.ds(SUBLANES, SUBLANES)]
            pltpu.make_async_copy(part, part, y_recv.at[k, 1]).wait()

        x_filter([yb[k, c] for c in range(nx)], put_edge)
        y_weights = jnp.concatenate([y_own, y_own], 1)
        e_weights = jnp.concatenate([y_edge, y_edge], 1)
        for c in range(nx):
            at = pl.ds(c * columns, columns)
            stage[k, :, at] = dot(y_weights, xs[pl.ds(0, 2 * rows), at]) + dot(
                e_weights, xs[pl.ds(2 * rows, 4 * SUBLANES), at]
            )
        finish(k).start()
        return carry

    lax.fori_loop(0, layers, take_step, 0)

    @pl.when(has_down)
    def _():
        for j in range(RADIUS):
            to_next(j).wait_send()

    @pl.when(has_up)
    def _():
        for j in range(RADIUS):
            to_previous(j).wait_send()

    def settle(k, carry):
        for p in range(nx):

            @pl.when(gx != p)
            def _():
                piece(k, p, 0).wait_send()

        finish(k).wait()
        return carry

    lax.fori_loop(0, layers, settle, 0)


def filtered_sums(sizes, density, mask):
    planes, rows, columns = density.shape
    nz, nx, ny = sizes
    layers = planes // nx
    blocks = mask.shape[0]
    width = nx * columns
    dma = pltpu.SemaphoreType.DMA
    return pl.pallas_call(
        functools.partial(kernel, sizes),
        out_shape=jax.ShapeDtypeStruct((layers, rows, width), jnp.float32),
        in_specs=[pl.BlockSpec(memory_space=pl.ANY)] * 2,
        out_specs=pl.BlockSpec(memory_space=pl.ANY),
        scratch_shapes=[
            pltpu.VMEM((planes + 2 * RADIUS, rows, columns), jnp.float32),
            pltpu.VMEM((blocks + 2, rows, columns), jnp.float32),
            pltpu.VMEM((blocks + 2,) + mask.shape[1:], jnp.int32),
            pltpu.VMEM((planes, rows, columns), jnp.float32),
            pltpu.VMEM((layers, nx, rows, columns), jnp.float32),
            pltpu.VMEM((layers, nx, 2 * SUBLANES, columns), jnp.float32),
            pltpu.VMEM((2 * rows + 4 * SUBLANES, width), jnp.bfloat16),
            pltpu.VMEM((layers, rows, width), jnp.float32),
            pltpu.VMEM((columns, columns), jnp.bfloat16),
            pltpu.VMEM((2 * LANES, columns), jnp.bfloat16),
            dma((blocks,)),
            dma,
            dma((2,)),
            dma((2,)),
            dma((2, RADIUS)),
            dma((2, RADIUS)),
            dma((layers, nx)),
            dma((layers, nx)),
            dma((layers, 2)),
            dma((layers, 2)),
            dma((layers,)),
        ],
        compiler_params=pltpu.CompilerParams(
            collective_id=0, has_side_effects=True, vmem_limit_bytes=48 * 1024 * 1024
        ),
    )(density, mask)


def one_side(reach):
    return reach * (RADIUS + 1) - reach * (reach + 1) // 2


def edge_sums(start, length, length_all):
    position = start + lax.iota(jnp.int32, length)
    reach_left = jnp.minimum(position, RADIUS)
    reach_right = jnp.minimum(length_all - 1 - position, RADIUS)
    return (RADIUS + 1 + one_side(reach_left) + one_side(reach_right)).astype(jnp.float32)


def body(sizes, density, mask):
    planes, rows, columns = density.shape
    nz, nx, ny = sizes
    layers = planes // nx
    summed = filtered_sums(sizes, density, mask)
    scale_x = 1.0 / edge_sums(0, columns * nx, columns * nx)
    scale_y = 1.0 / edge_sums(lax.axis_index("gy") * rows, rows, rows * ny)
    scale_z = 1.0 / edge_sums(lax.axis_index(("gz", "gx")) * layers, layers, planes * nz)
    scale = scale_z[:, None, None] * scale_y[None, :, None] * scale_x[None, None, :]
    filtered = summed * scale
    top = math.tanh(sharpness * threshold)
    bottom = top + math.tanh(sharpness * (1.0 - threshold))
    projected = (top + jnp.tanh(sharpness * (filtered - threshold))) * (1.0 / bottom)
    return (filtered, projected)


def solution(mesh):
    sizes = (mesh.shape["gz"], mesh.shape["gx"], mesh.shape["gy"])
    placed = (P("gz", "gy", "gx"), P("gz", "gy", "gx"))
    return jax.shard_map(
        functools.partial(body, sizes),
        mesh=mesh,
        in_specs=placed,
        out_specs=(P(("gz", "gx"), "gy", None), P(("gz", "gx"), "gy", None)),
        check_vma=False,
    )
```

```python
import functools
import math

import jax
import jax.numpy as jnp
from jax import lax
from jax.experimental import pallas as pl
from jax.experimental.pallas import tpu as pltpu
from jax.sharding import PartitionSpec as P

RADIUS = 6
CELLS = 8
LANES = 128
SUBLANES = 8

sharpness = 8.0
threshold = 0.5
MESH = pl.DeviceIdType.MESH


def hat(rows, cols, offset):
    row = lax.broadcasted_iota(jnp.int32, (rows, cols), 0)
    col = lax.broadcasted_iota(jnp.int32, (rows, cols), 1)
    return jnp.maximum(RADIUS + 1 - jnp.abs(col + offset - row), 0).astype(jnp.float32)


def halves(values):
    high = values.astype(jnp.bfloat16)
    low = (values - high.astype(jnp.float32)).astype(jnp.bfloat16)
    return high, low


def projection(filtered):
    top = math.tanh(sharpness * threshold)
    bottom = top + math.tanh(sharpness * (1.0 - threshold))
    return (top + jnp.tanh(sharpness * (filtered - threshold))) * (1.0 / bottom)


def one_side(reach):
    return reach * (RADIUS + 1) - reach * (reach + 1) // 2


def dot(a, b):
    return jnp.dot(a, b, preferred_element_type=jnp.float32)


def x_filter(chunks, w_own, w_edge, xs, first):
    size, columns = chunks[0].shape
    high, low = zip(*[halves(chunk) for chunk in chunks])
    none = jnp.zeros((size, LANES), jnp.bfloat16)
    for c in range(len(chunks)):
        total = dot(high[c], w_own[...]) + dot(low[c], w_own[...])
        for part in (high, low):
            left = part[c - 1][:, columns - LANES :] if c > 0 else none
            right = part[c + 1][:, :LANES] if c < len(chunks) - 1 else none
            total = total + dot(jnp.concatenate([left, right], 1), w_edge[...])
        at = pl.ds(c * columns, columns)
        xs[pl.ds(first, size), at], xs[pl.ds(first + size, size), at] = halves(total)


def y_filter(xs, scale, scale_z, columns, put):
    rows, width = scale.shape
    own = hat(rows, rows, 0).astype(jnp.bfloat16)
    edge = jnp.concatenate([hat(rows, SUBLANES, -SUBLANES), hat(rows, SUBLANES, rows)], 1)
    edge = edge.astype(jnp.bfloat16)
    own = jnp.concatenate([own, own], 1)
    edge = jnp.concatenate([edge, edge], 1)
    for c in range(width // columns):
        at = pl.ds(c * columns, columns)
        summed = dot(own, xs[pl.ds(0, 2 * rows), at])
        summed = summed + dot(edge, xs[pl.ds(2 * rows, 4 * SUBLANES), at])
        put(at, summed * (scale[:, at] * scale_z))


def inverse_count(position, length):
    left = one_side(jnp.minimum(position, RADIUS))
    right = one_side(jnp.minimum(length - 1 - position, RADIUS))
    return 1.0 / (RADIUS + 1 + left + right).astype(jnp.float32)


def layer_of(k, layers):
    return jnp.where(lax.axis_index("gx") == 0, layers - 1 - k, k)


def scale_along_z(sizes, k, layers, columns):
    nz, nx, ny = sizes
    level = (lax.axis_index("gz") * nx + lax.axis_index("gx")) * layers + layer_of(k, layers)
    level = jnp.full((SUBLANES, columns), level, jnp.int32)
    return inverse_count(level, nz * nx * layers)[0:1]


def kernel(
    sizes,
    density,
    mask,
    fstage,
    pstage,
    lrecv,
    lyb,
    scale,
    w_own,
    w_edge,
    phys,
    codes,
    masks,
    zf,
    recv,
    yb,
    xs,
    load_sem,
    mask_sem,
    hmask_send,
    hmask_recv,
    halo_send,
    halo_recv,
    send_sem,
    recv_sem,
    y_send,
    y_recv,
    e_send,
    e_recv,
):
    nz, nx, ny = sizes
    planes, rows, columns = density.shape
    blocks = mask.shape[0]
    layers = planes // nx
    gz, gx, gy = lax.axis_index("gz"), lax.axis_index("gx"), lax.axis_index("gy")
    has_up, has_down = gz > 0, gz < nz - 1
    has_prev, has_next = gy > 0, gy < ny - 1

    def load(b):
        part = pl.ds(b * CELLS, CELLS)
        return pltpu.make_async_copy(
            density.at[part], phys.at[pl.ds(RADIUS + b * CELLS, CELLS)], load_sem.at[b]
        )

    mask_copy = pltpu.make_async_copy(mask, masks.at[pl.ds(1, blocks)], mask_sem)
    mask_copy.start()
    for b in range(blocks):
        load(b).start()

    barrier = pltpu.get_barrier_semaphore()

    def greet(**where):
        pl.semaphore_signal(barrier, inc=1, device_id=where, device_id_type=MESH)

    pl.when(has_up)(lambda: greet(gz=gz - 1))
    pl.when(has_down)(lambda: greet(gz=gz + 1))
    pl.when(has_prev)(lambda: greet(gy=gy - 1))
    pl.when(has_next)(lambda: greet(gy=gy + 1))
    for step in range(1, nx):
        greet(gx=lax.rem(gx + step, nx))

    def to_next(j):
        return pltpu.make_async_remote_copy(
            src_ref=density.at[planes - 1 - j],
            dst_ref=phys.at[RADIUS - 1 - j],
            send_sem=halo_send.at[0, j],
            recv_sem=halo_recv.at[0, j],
            device_id={"gz": gz + 1},
            device_id_type=MESH,
        )

    def to_previous(j):
        return pltpu.make_async_remote_copy(
            src_ref=density.at[j],
            dst_ref=phys.at[RADIUS + planes + j],
            send_sem=halo_send.at[1, j],
            recv_sem=halo_recv.at[1, j],
            device_id={"gz": gz - 1},
            device_id_type=MESH,
        )

    def mask_next():
        return pltpu.make_async_remote_copy(
            src_ref=mask.at[blocks - 1],
            dst_ref=masks.at[0],
            send_sem=hmask_send.at[0],
            recv_sem=hmask_recv.at[0],
            device_id={"gz": gz + 1},
            device_id_type=MESH,
        )

    def mask_previous():
        return pltpu.make_async_remote_copy(
            src_ref=mask.at[0],
            dst_ref=masks.at[blocks + 1],
            send_sem=hmask_send.at[1],
            recv_sem=hmask_recv.at[1],
            device_id={"gz": gz - 1},
            device_id_type=MESH,
        )

    def spread(b):
        small = masks[b].astype(jnp.float32).astype(jnp.bfloat16)
        mrows, mcols = small.shape
        r = lax.broadcasted_iota(jnp.int32, (rows, mrows), 0) // CELLS
        m = lax.broadcasted_iota(jnp.int32, (rows, mrows), 1)
        tall = dot(jnp.where(r == m, 1.0, 0.0).astype(jnp.bfloat16), small)
        c = lax.broadcasted_iota(jnp.int32, (mcols, columns), 1) // CELLS
        n = lax.broadcasted_iota(jnp.int32, (mcols, columns), 0)
        wide = jnp.where(c == n, 1.0, 0.0).astype(jnp.bfloat16)
        codes[b] = dot(tall.astype(jnp.bfloat16), wide)

    def apply_mask(row, b):
        code = codes[b]
        phys[row] = jnp.where(code < 0.5, 0.0, jnp.where(code < 1.5, 1.0, phys[row]))

    def piece(k, p, row):
        return pltpu.make_async_remote_copy(
            src_ref=zf.at[row],
            dst_ref=recv.at[k, gx],
            send_sem=send_sem.at[k, p],
            recv_sem=recv_sem.at[k, gx],
            device_id={"gx": p},
            device_id_type=MESH,
        )

    edges = (pl.ds(0, SUBLANES), pl.ds(rows - SUBLANES, SUBLANES))
    inside = pl.ds(SUBLANES, rows - 2 * SUBLANES)

    def edge_piece(side, p, row):
        return pltpu.make_async_remote_copy(
            src_ref=zf.at[row, edges[side]],
            dst_ref=lrecv.at[gx, edges[side]],
            send_sem=e_send.at[side, p],
            recv_sem=e_recv.at[side, gx],
            device_id={"gx": p},
            device_id_type=MESH,
        )

    def inner_piece(p, row):
        return pltpu.make_async_remote_copy(
            src_ref=zf.at[row, inside],
            dst_ref=lrecv.at[gx, inside],
            send_sem=send_sem.at[layers - 1, p],
            recv_sem=recv_sem.at[layers - 1, gx],
            device_id={"gx": p},
            device_id_type=MESH,
        )

    def row_of(k, p):
        return layers - 1 - k if p == 0 else p * layers + k

    def z_filter(row):
        part = rows // 4
        for i in range(4):
            at = pl.ds(i * part, part)
            run = phys[row + RADIUS, at]
            total = run
            for d in range(1, RADIUS + 1):
                run = run + (phys[row + RADIUS - d, at] + phys[row + RADIUS + d, at])
                total = total + run
            zf[row, at] = total

    def z_send(k, p):
        row = row_of(k, p)
        z_filter(row)

        @pl.when(gx != p)
        def _():
            piece(k, p, row).start()

        @pl.when(gx == p)
        def _():
            pltpu.make_async_copy(zf.at[row], recv.at[k, gx], recv_sem.at[k, gx]).start()

    def z_step(k, carry):
        for p in range(nx):
            z_send(k, p)
        return carry

    def mask_block(b):
        spread(b + 1)
        load(b).wait()

        def one(i, carry):
            apply_mask(RADIUS + b * CELLS + i, b + 1)
            return carry

        lax.fori_loop(0, CELLS, one, 0)

    mask_copy.wait()
    ready = 0
    for p in range(nx):
        need = min(blocks, (row_of(0, p) + RADIUS) // CELLS + 1)
        for b in range(ready, need):
            mask_block(b)
        if p == 0:
            count = nx - 1
            for there in (has_up, has_down, has_prev, has_next):
                count = count + there.astype(jnp.int32)
            pl.semaphore_wait(barrier, count)
        ready = max(ready, need)
        z_send(0, p)
    for b in range(ready, blocks):
        mask_block(b)

    @pl.when(has_down)
    def _():
        mask_next().start()
        for j in range(RADIUS):
            to_next(j).start()

    @pl.when(has_up)
    def _():
        mask_previous().start()
        for j in range(RADIUS):
            to_previous(j).start()

    @pl.when(jnp.logical_not(has_up))
    def _():
        phys[pl.ds(0, RADIUS)] = jnp.zeros((RADIUS, rows, columns), jnp.float32)

    @pl.when(jnp.logical_not(has_down))
    def _():
        phys[pl.ds(RADIUS + planes, RADIUS)] = jnp.zeros((RADIUS, rows, columns), jnp.float32)

    @pl.when(jnp.logical_not(has_prev))
    def _():
        lyb[:, pl.ds(0, SUBLANES)] = jnp.zeros((nx, SUBLANES, columns), jnp.float32)
        yb[:, :, pl.ds(0, SUBLANES)] = jnp.zeros((layers - 1, nx, SUBLANES, columns), jnp.float32)

    @pl.when(jnp.logical_not(has_next))
    def _():
        lyb[:, pl.ds(SUBLANES, SUBLANES)] = jnp.zeros((nx, SUBLANES, columns), jnp.float32)
        yb[:, :, pl.ds(SUBLANES, SUBLANES)] = jnp.zeros((layers - 1, nx, SUBLANES, columns), jnp.float32)

    free = layers - RADIUS
    lax.fori_loop(1, free, z_step, 0)

    w_own[...] = hat(columns, columns, 0).astype(jnp.bfloat16)
    w_edge[pl.ds(0, LANES)] = hat(LANES, columns, LANES).astype(jnp.bfloat16)
    w_edge[pl.ds(LANES, LANES)] = hat(LANES, columns, -columns).astype(jnp.bfloat16)

    width = nx * columns
    scale_y = inverse_count(
        gy * rows + lax.broadcasted_iota(jnp.int32, (rows, LANES), 0), rows * ny
    )
    for c in range(0, width, LANES):
        lane = c + lax.broadcasted_iota(jnp.int32, (SUBLANES, LANES), 1)
        scale_x = inverse_count(lane, width)
        scale[:, pl.ds(c, LANES)] = scale_y * scale_x[0:1]

    @pl.when(has_up)
    def _():
        mask_previous().wait_send()
        pltpu.make_async_copy(mask.at[0], masks.at[0], hmask_recv.at[0]).wait()
        spread(0)

    @pl.when(has_down)
    def _():
        mask_next().wait_send()
        pltpu.make_async_copy(mask.at[0], masks.at[blocks + 1], hmask_recv.at[1]).wait()
        spread(blocks + 1)

    def take_halo(k):
        j = k - free

        @pl.when(has_up)
        def _():
            row = RADIUS - 1 - j
            pltpu.make_async_copy(density.at[0], phys.at[row], halo_recv.at[0, j]).wait()
            apply_mask(row, 0)

        @pl.when(has_down)
        def _():
            row = RADIUS + planes + j
            pltpu.make_async_copy(density.at[0], phys.at[row], halo_recv.at[1, j]).wait()
            apply_mask(row, blocks + 1)

    def halo_step(k, carry):
        take_halo(k)
        return z_step(k, carry)

    final = layers - 1
    lax.fori_loop(free, final, halo_step, 0)

    take_halo(final)
    for p in range(nx):
        row = row_of(final, p)
        z_filter(row)

        @pl.when(gx != p)
        def _():
            edge_piece(0, p, row).start()
            edge_piece(1, p, row).start()

        @pl.when(gx == p)
        def _():
            for side in range(2):
                pltpu.make_async_copy(
                    zf.at[row, edges[side]], lrecv.at[gx, edges[side]], e_recv.at[side, gx]
                ).start()
            pltpu.make_async_copy(
                zf.at[row, inside], lrecv.at[gx, inside], recv_sem.at[final, gx]
            ).start()

    for p in range(nx):

        @pl.when(gx != p)
        def _():
            inner_piece(p, row_of(final, p)).start()

    def y_previous(k):
        return pltpu.make_async_remote_copy(
            src_ref=recv.at[k, :, pl.ds(0, SUBLANES)],
            dst_ref=yb.at[k, :, pl.ds(SUBLANES, SUBLANES)],
            send_sem=y_send.at[k, 0],
            recv_sem=y_recv.at[k, 1],
            device_id={"gy": gy - 1},
            device_id_type=MESH,
        )

    def y_next(k):
        return pltpu.make_async_remote_copy(
            src_ref=recv.at[k, :, pl.ds(rows - SUBLANES, SUBLANES)],
            dst_ref=yb.at[k, :, pl.ds(0, SUBLANES)],
            send_sem=y_send.at[k, 1],
            recv_sem=y_recv.at[k, 0],
            device_id={"gy": gy + 1},
            device_id_type=MESH,
        )

    def last_previous():
        return pltpu.make_async_remote_copy(
            src_ref=lrecv.at[:, pl.ds(0, SUBLANES)],
            dst_ref=lyb.at[:, pl.ds(SUBLANES, SUBLANES)],
            send_sem=y_send.at[final, 0],
            recv_sem=y_recv.at[final, 1],
            device_id={"gy": gy - 1},
            device_id_type=MESH,
        )

    def last_next():
        return pltpu.make_async_remote_copy(
            src_ref=lrecv.at[:, pl.ds(rows - SUBLANES, SUBLANES)],
            dst_ref=lyb.at[:, pl.ds(0, SUBLANES)],
            send_sem=y_send.at[final, 1],
            recv_sem=y_recv.at[final, 0],
            device_id={"gy": gy + 1},
            device_id_type=MESH,
        )

    def send_edges(k):
        pl.when(has_prev)(lambda: y_previous(k).start())
        pl.when(has_next)(lambda: y_next(k).start())

    def take_edges(k):
        @pl.when(has_prev)
        def _():
            y_previous(k).wait_send()
            part = yb.at[k, :, pl.ds(0, SUBLANES)]
            pltpu.make_async_copy(part, part, y_recv.at[k, 0]).wait()

        @pl.when(has_next)
        def _():
            y_next(k).wait_send()
            part = yb.at[k, :, pl.ds(SUBLANES, SUBLANES)]
            pltpu.make_async_copy(part, part, y_recv.at[k, 1]).wait()

    def take_step(k, carry):
        for c in range(nx):
            pltpu.make_async_copy(zf.at[0], recv.at[k, c], recv_sem.at[k, c]).wait()
        send_edges(k)
        x_filter([recv[k, c] for c in range(nx)], w_own, w_edge, xs, 0)
        take_edges(k)
        x_filter([yb[k, c] for c in range(nx)], w_own, w_edge, xs, 2 * rows)

        def put(at, value):
            fstage[k, :, at] = value
            pstage[k, :, at] = projection(value)

        y_filter(xs, scale, scale_along_z(sizes, k, layers, columns), columns, put)
        return carry

    lax.fori_loop(0, final, take_step, 0)

    for c in range(nx):
        for side in range(2):
            part = lrecv.at[c, edges[side]]
            pltpu.make_async_copy(part, part, e_recv.at[side, c]).wait()
    pl.when(has_prev)(lambda: last_previous().start())
    pl.when(has_next)(lambda: last_next().start())

    @pl.when(has_down)
    def _():
        for j in range(RADIUS):
            to_next(j).wait_send()

    @pl.when(has_up)
    def _():
        for j in range(RADIUS):
            to_previous(j).wait_send()

    def settle(k, carry):
        for p in range(nx):

            @pl.when(gx != p)
            def _():
                piece(k, p, 0).wait_send()

        return carry

    lax.fori_loop(0, final, settle, 0)
    for p in range(nx):

        @pl.when(gx != p)
        def _():
            edge_piece(0, p, 0).wait_send()
            edge_piece(1, p, 0).wait_send()
            inner_piece(p, 0).wait_send()

    @pl.when(has_prev)
    def _():
        last_previous().wait_send()
        part = lyb.at[:, pl.ds(0, SUBLANES)]
        pltpu.make_async_copy(part, part, y_recv.at[final, 0]).wait()

    @pl.when(has_next)
    def _():
        last_next().wait_send()
        part = lyb.at[:, pl.ds(SUBLANES, SUBLANES)]
        pltpu.make_async_copy(part, part, y_recv.at[final, 1]).wait()

    for c in range(nx):
        part = lrecv.at[c, inside]
        pltpu.make_async_copy(part, part, recv_sem.at[final, c]).wait()


def closing(sizes, fstage, pstage, lrecv, lyb, scale, w_own, w_edge, filt, proj, xs, flast, plast, sems, last_sems):
    final = fstage.shape[0]
    nx, rows, columns = lrecv.shape
    layers = final + 1

    def finished(k):
        at = layer_of(k, layers)
        return (
            pltpu.make_async_copy(fstage.at[k], filt.at[at], sems.at[0, k]),
            pltpu.make_async_copy(pstage.at[k], proj.at[at], sems.at[1, k]),
        )

    for k in range(final):
        for copy in finished(k):
            copy.start()
    x_filter([lrecv[c] for c in range(nx)], w_own, w_edge, xs, 0)
    x_filter([lyb[c] for c in range(nx)], w_own, w_edge, xs, 2 * rows)

    def put(at, value):
        flast[:, at] = value
        plast[:, at] = projection(value)

    y_filter(xs, scale, scale_along_z(sizes, final, layers, columns), columns, put)
    at = layer_of(final, layers)
    ends = (
        pltpu.make_async_copy(flast, filt.at[at], last_sems.at[0]),
        pltpu.make_async_copy(plast, proj.at[at], last_sems.at[1]),
    )
    for copy in ends:
        copy.start()
    for k in range(final):
        for copy in finished(k):
            copy.wait()
    for copy in ends:
        copy.wait()


def body(sizes, density, mask):
    planes, rows, columns = density.shape
    nz, nx, ny = sizes
    layers = planes // nx
    final = layers - 1
    blocks = mask.shape[0]
    width = nx * columns
    dma = pltpu.SemaphoreType.DMA
    f32, bf16 = jnp.float32, jnp.bfloat16
    shape = jax.ShapeDtypeStruct
    carried = (
        shape((final, rows, width), f32),
        shape((final, rows, width), f32),
        shape((nx, rows, columns), f32),
        shape((nx, 2 * SUBLANES, columns), f32),
        shape((rows, width), f32),
        shape((columns, columns), bf16),
        shape((2 * LANES, columns), bf16),
    )
    xs = pltpu.VMEM((2 * rows + 4 * SUBLANES, width), bf16)
    held = pl.pallas_call(
        functools.partial(kernel, sizes),
        out_shape=carried,
        in_specs=[pl.BlockSpec(memory_space=pl.ANY)] * 2,
        out_specs=(pl.BlockSpec(memory_space=pltpu.VMEM),) * len(carried),
        scratch_shapes=[
            pltpu.VMEM((planes + 2 * RADIUS, rows, columns), f32),
            pltpu.VMEM((blocks + 2, rows, columns), f32),
            pltpu.VMEM((blocks + 2,) + mask.shape[1:], jnp.int32),
            pltpu.VMEM((planes, rows, columns), f32),
            pltpu.VMEM((final, nx, rows, columns), f32),
            pltpu.VMEM((final, nx, 2 * SUBLANES, columns), f32),
            xs,
            dma((blocks,)),
            dma,
            dma((2,)),
            dma((2,)),
            dma((2, RADIUS)),
            dma((2, RADIUS)),
            dma((layers, nx)),
            dma((layers, nx)),
            dma((layers, 2)),
            dma((layers, 2)),
            dma((2, nx)),
            dma((2, nx)),
        ],
        compiler_params=pltpu.CompilerParams(
            collective_id=0, has_side_effects=True, vmem_limit_bytes=44 * 1024 * 1024
        ),
    )(density, mask)
    return pl.pallas_call(
        functools.partial(closing, sizes),
        out_shape=(shape((layers, rows, width), f32),) * 2,
        in_specs=[pl.BlockSpec(memory_space=pltpu.VMEM)] * len(carried),
        out_specs=(pl.BlockSpec(memory_space=pl.ANY),) * 2,
        scratch_shapes=[
            xs,
            pltpu.VMEM((rows, width), f32),
            pltpu.VMEM((rows, width), f32),
            dma((2, final)),
            dma((2,)),
        ],
        compiler_params=pltpu.CompilerParams(vmem_limit_bytes=16 * 1024 * 1024),
    )(*held)


def solution(mesh):
    sizes = (mesh.shape["gz"], mesh.shape["gx"], mesh.shape["gy"])
    placed = (P("gz", "gy", "gx"), P("gz", "gy", "gx"))
    return jax.shard_map(
        functools.partial(body, sizes),
        mesh=mesh,
        in_specs=placed,
        out_specs=(P(("gz", "gx"), "gy", None), P(("gz", "gx"), "gy", None)),
        check_vma=False,
    )
```

```python
import functools
import math

import jax
import jax.numpy as jnp
from jax import lax
from jax.experimental import pallas as pl
from jax.experimental.pallas import tpu as pltpu
from jax.sharding import PartitionSpec as P

RADIUS = 6
CELLS = 8
LANES = 128
SUBLANES = 8

sharpness = 8.0
threshold = 0.5
MESH = pl.DeviceIdType.MESH


def hat(rows, cols, offset):
    row = lax.broadcasted_iota(jnp.int32, (rows, cols), 0)
    col = lax.broadcasted_iota(jnp.int32, (rows, cols), 1)
    return jnp.maximum(RADIUS + 1 - jnp.abs(col + offset - row), 0).astype(jnp.float32)


def halves(values):
    high = values.astype(jnp.bfloat16)
    low = (values - high.astype(jnp.float32)).astype(jnp.bfloat16)
    return high, low


def projection(filtered):
    top = math.tanh(sharpness * threshold)
    bottom = top + math.tanh(sharpness * (1.0 - threshold))
    return (top + jnp.tanh(sharpness * (filtered - threshold))) * (1.0 / bottom)


def one_side(reach):
    return reach * (RADIUS + 1) - reach * (reach + 1) // 2


def dot(a, b):
    return jnp.dot(a, b, preferred_element_type=jnp.float32)


def x_filter(chunks, w_own, w_edge, xs, first):
    size, columns = chunks[0].shape
    high, low = zip(*[halves(chunk) for chunk in chunks])
    none = jnp.zeros((size, LANES), jnp.bfloat16)
    for c in range(len(chunks)):
        total = dot(high[c], w_own[...]) + dot(low[c], w_own[...])
        for part in (high, low):
            left = part[c - 1][:, columns - LANES :] if c > 0 else none
            right = part[c + 1][:, :LANES] if c < len(chunks) - 1 else none
            total = total + dot(jnp.concatenate([left, right], 1), w_edge[...])
        at = pl.ds(c * columns, columns)
        xs[pl.ds(first, size), at], xs[pl.ds(first + size, size), at] = halves(total)


def y_filter(xs, scale, scale_z, columns, put):
    rows, width = scale.shape
    own = hat(rows, rows, 0).astype(jnp.bfloat16)
    edge = jnp.concatenate([hat(rows, SUBLANES, -SUBLANES), hat(rows, SUBLANES, rows)], 1)
    edge = edge.astype(jnp.bfloat16)
    own = jnp.concatenate([own, own], 1)
    edge = jnp.concatenate([edge, edge], 1)
    for c in range(width // columns):
        at = pl.ds(c * columns, columns)
        summed = dot(own, xs[pl.ds(0, 2 * rows), at])
        summed = summed + dot(edge, xs[pl.ds(2 * rows, 4 * SUBLANES), at])
        put(at, summed * (scale[:, at] * scale_z))


def inverse_count(position, length):
    left = one_side(jnp.minimum(position, RADIUS))
    right = one_side(jnp.minimum(length - 1 - position, RADIUS))
    return 1.0 / (RADIUS + 1 + left + right).astype(jnp.float32)


def layer_of(k, layers):
    return jnp.where(lax.axis_index("gx") == 0, layers - 1 - k, k)


def scale_along_z(sizes, k, layers, columns):
    nz, nx, ny = sizes
    level = (lax.axis_index("gz") * nx + lax.axis_index("gx")) * layers + layer_of(k, layers)
    level = jnp.full((SUBLANES, columns), level, jnp.int32)
    return inverse_count(level, nz * nx * layers)[0:1]


def kernel(
    sizes,
    density,
    mask,
    fstage,
    pstage,
    lrecv,
    lyb,
    scale,
    w_own,
    w_edge,
    phys,
    codes,
    masks,
    zf,
    recv,
    yb,
    xs,
    load_sem,
    mask_sem,
    hmask_send,
    hmask_recv,
    halo_send,
    halo_recv,
    send_sem,
    recv_sem,
    y_send,
    y_recv,
    e_send,
    e_recv,
):
    nz, nx, ny = sizes
    planes, rows, columns = density.shape
    blocks = mask.shape[0]
    layers = planes // nx
    gz, gx, gy = lax.axis_index("gz"), lax.axis_index("gx"), lax.axis_index("gy")
    has_up, has_down = gz > 0, gz < nz - 1
    has_prev, has_next = gy > 0, gy < ny - 1

    def load(b):
        part = pl.ds(b * CELLS, CELLS)
        return pltpu.make_async_copy(
            density.at[part], phys.at[pl.ds(RADIUS + b * CELLS, CELLS)], load_sem.at[b]
        )

    mask_copy = pltpu.make_async_copy(mask, masks.at[pl.ds(1, blocks)], mask_sem)
    mask_copy.start()
    for b in range(blocks):
        load(b).start()

    barrier = pltpu.get_barrier_semaphore()

    def greet(**where):
        pl.semaphore_signal(barrier, inc=1, device_id=where, device_id_type=MESH)

    pl.when(has_up)(lambda: greet(gz=gz - 1))
    pl.when(has_down)(lambda: greet(gz=gz + 1))
    pl.when(has_prev)(lambda: greet(gy=gy - 1))
    pl.when(has_next)(lambda: greet(gy=gy + 1))
    for step in range(1, nx):
        greet(gx=lax.rem(gx + step, nx))

    def to_next(j):
        return pltpu.make_async_remote_copy(
            src_ref=density.at[planes - 1 - j],
            dst_ref=phys.at[RADIUS - 1 - j],
            send_sem=halo_send.at[0, j],
            recv_sem=halo_recv.at[0, j],
            device_id={"gz": gz + 1},
            device_id_type=MESH,
        )

    def to_previous(j):
        return pltpu.make_async_remote_copy(
            src_ref=density.at[j],
            dst_ref=phys.at[RADIUS + planes + j],
            send_sem=halo_send.at[1, j],
            recv_sem=halo_recv.at[1, j],
            device_id={"gz": gz - 1},
            device_id_type=MESH,
        )

    def mask_next():
        return pltpu.make_async_remote_copy(
            src_ref=mask.at[blocks - 1],
            dst_ref=masks.at[0],
            send_sem=hmask_send.at[0],
            recv_sem=hmask_recv.at[0],
            device_id={"gz": gz + 1},
            device_id_type=MESH,
        )

    def mask_previous():
        return pltpu.make_async_remote_copy(
            src_ref=mask.at[0],
            dst_ref=masks.at[blocks + 1],
            send_sem=hmask_send.at[1],
            recv_sem=hmask_recv.at[1],
            device_id={"gz": gz - 1},
            device_id_type=MESH,
        )

    def spread(b):
        small = masks[b].astype(jnp.float32).astype(jnp.bfloat16)
        mrows, mcols = small.shape
        r = lax.broadcasted_iota(jnp.int32, (rows, mrows), 0) // CELLS
        m = lax.broadcasted_iota(jnp.int32, (rows, mrows), 1)
        tall = dot(jnp.where(r == m, 1.0, 0.0).astype(jnp.bfloat16), small)
        c = lax.broadcasted_iota(jnp.int32, (mcols, columns), 1) // CELLS
        n = lax.broadcasted_iota(jnp.int32, (mcols, columns), 0)
        wide = jnp.where(c == n, 1.0, 0.0).astype(jnp.bfloat16)
        codes[b] = dot(tall.astype(jnp.bfloat16), wide)

    def apply_mask(row, b):
        code = codes[b]
        phys[row] = jnp.where(code < 0.5, 0.0, jnp.where(code < 1.5, 1.0, phys[row]))

    def piece(k, p, row):
        return pltpu.make_async_remote_copy(
            src_ref=zf.at[row],
            dst_ref=recv.at[k, gx],
            send_sem=send_sem.at[k, p],
            recv_sem=recv_sem.at[k, gx],
            device_id={"gx": p},
            device_id_type=MESH,
        )

    edges = (pl.ds(0, SUBLANES), pl.ds(rows - SUBLANES, SUBLANES))
    inside = pl.ds(SUBLANES, rows - 2 * SUBLANES)

    def edge_piece(side, p, row):
        return pltpu.make_async_remote_copy(
            src_ref=zf.at[row, edges[side]],
            dst_ref=lrecv.at[gx, edges[side]],
            send_sem=e_send.at[side, p],
            recv_sem=e_recv.at[side, gx],
            device_id={"gx": p},
            device_id_type=MESH,
        )

    def inner_piece(p, row):
        return pltpu.make_async_remote_copy(
            src_ref=zf.at[row, inside],
            dst_ref=lrecv.at[gx, inside],
            send_sem=send_sem.at[layers - 1, p],
            recv_sem=recv_sem.at[layers - 1, gx],
            device_id={"gx": p},
            device_id_type=MESH,
        )

    def row_of(k, p):
        return layers - 1 - k if p == 0 else p * layers + k

    def z_filter(row):
        part = rows // 4
        for i in range(4):
            at = pl.ds(i * part, part)
            run = phys[row + RADIUS, at]
            total = run
            for d in range(1, RADIUS + 1):
                run = run + (phys[row + RADIUS - d, at] + phys[row + RADIUS + d, at])
                total = total + run
            zf[row, at] = total

    def z_send(k, p):
        row = row_of(k, p)
        z_filter(row)

        @pl.when(gx != p)
        def _():
            piece(k, p, row).start()

        @pl.when(gx == p)
        def _():
            pltpu.make_async_copy(zf.at[row], recv.at[k, gx], recv_sem.at[k, gx]).start()

    def z_step(k, carry):
        for p in range(nx):
            z_send(k, p)
        return carry

    def mask_block(b):
        spread(b + 1)
        load(b).wait()

        def one(i, carry):
            apply_mask(RADIUS + b * CELLS + i, b + 1)
            return carry

        lax.fori_loop(0, CELLS, one, 0)

    mask_copy.wait()
    ready = 0
    for p in range(nx):
        need = min(blocks, (row_of(0, p) + RADIUS) // CELLS + 1)
        for b in range(ready, need):
            mask_block(b)
        if p == 0:
            count = nx - 1
            for there in (has_up, has_down, has_prev, has_next):
                count = count + there.astype(jnp.int32)
            pl.semaphore_wait(barrier, count)
        ready = max(ready, need)
        z_send(0, p)
    for b in range(ready, blocks):
        mask_block(b)

    @pl.when(has_down)
    def _():
        mask_next().start()
        for j in range(RADIUS):
            to_next(j).start()

    @pl.when(has_up)
    def _():
        mask_previous().start()
        for j in range(RADIUS):
            to_previous(j).start()

    @pl.when(jnp.logical_not(has_up))
    def _():
        phys[pl.ds(0, RADIUS)] = jnp.zeros((RADIUS, rows, columns), jnp.float32)

    @pl.when(jnp.logical_not(has_down))
    def _():
        phys[pl.ds(RADIUS + planes, RADIUS)] = jnp.zeros((RADIUS, rows, columns), jnp.float32)

    @pl.when(jnp.logical_not(has_prev))
    def _():
        lyb[:, pl.ds(0, SUBLANES)] = jnp.zeros((nx, SUBLANES, columns), jnp.float32)
        yb[:, :, pl.ds(0, SUBLANES)] = jnp.zeros((layers - 1, nx, SUBLANES, columns), jnp.float32)

    @pl.when(jnp.logical_not(has_next))
    def _():
        lyb[:, pl.ds(SUBLANES, SUBLANES)] = jnp.zeros((nx, SUBLANES, columns), jnp.float32)
        yb[:, :, pl.ds(SUBLANES, SUBLANES)] = jnp.zeros((layers - 1, nx, SUBLANES, columns), jnp.float32)

    free = layers - RADIUS
    lax.fori_loop(1, free, z_step, 0)

    w_own[...] = hat(columns, columns, 0).astype(jnp.bfloat16)
    w_edge[pl.ds(0, LANES)] = hat(LANES, columns, LANES).astype(jnp.bfloat16)
    w_edge[pl.ds(LANES, LANES)] = hat(LANES, columns, -columns).astype(jnp.bfloat16)

    width = nx * columns
    scale_y = inverse_count(
        gy * rows + lax.broadcasted_iota(jnp.int32, (rows, LANES), 0), rows * ny
    )
    for c in range(0, width, LANES):
        lane = c + lax.broadcasted_iota(jnp.int32, (SUBLANES, LANES), 1)
        scale_x = inverse_count(lane, width)
        scale[:, pl.ds(c, LANES)] = scale_y * scale_x[0:1]

    @pl.when(has_up)
    def _():
        mask_previous().wait_send()
        pltpu.make_async_copy(mask.at[0], masks.at[0], hmask_recv.at[0]).wait()
        spread(0)

    @pl.when(has_down)
    def _():
        mask_next().wait_send()
        pltpu.make_async_copy(mask.at[0], masks.at[blocks + 1], hmask_recv.at[1]).wait()
        spread(blocks + 1)

    def take_halo(k):
        j = k - free

        @pl.when(has_up)
        def _():
            row = RADIUS - 1 - j
            pltpu.make_async_copy(density.at[0], phys.at[row], halo_recv.at[0, j]).wait()
            apply_mask(row, 0)

        @pl.when(has_down)
        def _():
            row = RADIUS + planes + j
            pltpu.make_async_copy(density.at[0], phys.at[row], halo_recv.at[1, j]).wait()
            apply_mask(row, blocks + 1)

    def halo_step(k, carry):
        take_halo(k)
        return z_step(k, carry)

    final = layers - 1
    lax.fori_loop(free, final, halo_step, 0)

    take_halo(final)
    for p in range(nx):
        row = row_of(final, p)
        z_filter(row)

        @pl.when(gx != p)
        def _():
            edge_piece(0, p, row).start()
            edge_piece(1, p, row).start()

        @pl.when(gx == p)
        def _():
            for side in range(2):
                pltpu.make_async_copy(
                    zf.at[row, edges[side]], lrecv.at[gx, edges[side]], e_recv.at[side, gx]
                ).start()
            pltpu.make_async_copy(
                zf.at[row, inside], lrecv.at[gx, inside], recv_sem.at[final, gx]
            ).start()

    for p in range(nx):

        @pl.when(gx != p)
        def _():
            inner_piece(p, row_of(final, p)).start()

    def y_previous(k):
        return pltpu.make_async_remote_copy(
            src_ref=recv.at[k, :, pl.ds(0, SUBLANES)],
            dst_ref=yb.at[k, :, pl.ds(SUBLANES, SUBLANES)],
            send_sem=y_send.at[k, 0],
            recv_sem=y_recv.at[k, 1],
            device_id={"gy": gy - 1},
            device_id_type=MESH,
        )

    def y_next(k):
        return pltpu.make_async_remote_copy(
            src_ref=recv.at[k, :, pl.ds(rows - SUBLANES, SUBLANES)],
            dst_ref=yb.at[k, :, pl.ds(0, SUBLANES)],
            send_sem=y_send.at[k, 1],
            recv_sem=y_recv.at[k, 0],
            device_id={"gy": gy + 1},
            device_id_type=MESH,
        )

    def last_previous():
        return pltpu.make_async_remote_copy(
            src_ref=lrecv.at[:, pl.ds(0, SUBLANES)],
            dst_ref=lyb.at[:, pl.ds(SUBLANES, SUBLANES)],
            send_sem=y_send.at[final, 0],
            recv_sem=y_recv.at[final, 1],
            device_id={"gy": gy - 1},
            device_id_type=MESH,
        )

    def last_next():
        return pltpu.make_async_remote_copy(
            src_ref=lrecv.at[:, pl.ds(rows - SUBLANES, SUBLANES)],
            dst_ref=lyb.at[:, pl.ds(0, SUBLANES)],
            send_sem=y_send.at[final, 1],
            recv_sem=y_recv.at[final, 0],
            device_id={"gy": gy + 1},
            device_id_type=MESH,
        )

    def send_edges(k):
        pl.when(has_prev)(lambda: y_previous(k).start())
        pl.when(has_next)(lambda: y_next(k).start())

    def take_edges(k):
        @pl.when(has_prev)
        def _():
            y_previous(k).wait_send()
            part = yb.at[k, :, pl.ds(0, SUBLANES)]
            pltpu.make_async_copy(part, part, y_recv.at[k, 0]).wait()

        @pl.when(has_next)
        def _():
            y_next(k).wait_send()
            part = yb.at[k, :, pl.ds(SUBLANES, SUBLANES)]
            pltpu.make_async_copy(part, part, y_recv.at[k, 1]).wait()

    def take_step(k, carry):
        for c in range(nx):
            pltpu.make_async_copy(zf.at[0], recv.at[k, c], recv_sem.at[k, c]).wait()
        send_edges(k)
        x_filter([recv[k, c] for c in range(nx)], w_own, w_edge, xs, 0)
        take_edges(k)
        x_filter([yb[k, c] for c in range(nx)], w_own, w_edge, xs, 2 * rows)

        def put(at, value):
            fstage[k, :, at] = value
            pstage[k, :, at] = projection(value)

        y_filter(xs, scale, scale_along_z(sizes, k, layers, columns), columns, put)
        return carry

    lax.fori_loop(0, final, take_step, 0)

    for c in range(nx):
        for side in range(2):
            part = lrecv.at[c, edges[side]]
            pltpu.make_async_copy(part, part, e_recv.at[side, c]).wait()
    pl.when(has_prev)(lambda: last_previous().start())
    pl.when(has_next)(lambda: last_next().start())

    @pl.when(has_down)
    def _():
        for j in range(RADIUS):
            to_next(j).wait_send()

    @pl.when(has_up)
    def _():
        for j in range(RADIUS):
            to_previous(j).wait_send()

    def settle(k, carry):
        for p in range(nx):

            @pl.when(gx != p)
            def _():
                piece(k, p, 0).wait_send()

        return carry

    lax.fori_loop(0, final, settle, 0)
    for p in range(nx):

        @pl.when(gx != p)
        def _():
            edge_piece(0, p, 0).wait_send()
            edge_piece(1, p, 0).wait_send()
            inner_piece(p, 0).wait_send()

    @pl.when(has_prev)
    def _():
        last_previous().wait_send()
        part = lyb.at[:, pl.ds(0, SUBLANES)]
        pltpu.make_async_copy(part, part, y_recv.at[final, 0]).wait()

    @pl.when(has_next)
    def _():
        last_next().wait_send()
        part = lyb.at[:, pl.ds(SUBLANES, SUBLANES)]
        pltpu.make_async_copy(part, part, y_recv.at[final, 1]).wait()

    for c in range(nx):
        part = lrecv.at[c, inside]
        pltpu.make_async_copy(part, part, recv_sem.at[final, c]).wait()


def closing(sizes, fstage, pstage, lrecv, lyb, scale, w_own, w_edge, filt, proj, xs, flast, plast, sems, last_sems):
    final = fstage.shape[0]
    nx, rows, columns = lrecv.shape
    layers = final + 1

    def finished(k):
        at = layer_of(k, layers)
        return (
            pltpu.make_async_copy(fstage.at[k], filt.at[at], sems.at[0, k]),
            pltpu.make_async_copy(pstage.at[k], proj.at[at], sems.at[1, k]),
        )

    for k in range(final):
        for copy in finished(k):
            copy.start()
    x_filter([lrecv[c] for c in range(nx)], w_own, w_edge, xs, 0)
    x_filter([lyb[c] for c in range(nx)], w_own, w_edge, xs, 2 * rows)

    level = layer_of(final, layers)

    def ends(at):
        c = at.start // columns
        return (
            pltpu.make_async_copy(flast.at[:, at], filt.at[level, :, at], last_sems.at[0, c]),
            pltpu.make_async_copy(plast.at[:, at], proj.at[level, :, at], last_sems.at[1, c]),
        )

    def put(at, value):
        flast[:, at] = value
        first, second = ends(at)
        first.start()
        plast[:, at] = projection(value)
        second.start()

    y_filter(xs, scale, scale_along_z(sizes, final, layers, columns), columns, put)
    for k in range(final):
        for copy in finished(k):
            copy.wait()
    for c in range(nx):
        for copy in ends(pl.ds(c * columns, columns)):
            copy.wait()


def body(sizes, density, mask):
    planes, rows, columns = density.shape
    nz, nx, ny = sizes
    layers = planes // nx
    final = layers - 1
    blocks = mask.shape[0]
    width = nx * columns
    dma = pltpu.SemaphoreType.DMA
    f32, bf16 = jnp.float32, jnp.bfloat16
    shape = jax.ShapeDtypeStruct
    carried = (
        shape((final, rows, width), f32),
        shape((final, rows, width), f32),
        shape((nx, rows, columns), f32),
        shape((nx, 2 * SUBLANES, columns), f32),
        shape((rows, width), f32),
        shape((columns, columns), bf16),
        shape((2 * LANES, columns), bf16),
    )
    xs = pltpu.VMEM((2 * rows + 4 * SUBLANES, width), bf16)
    held = pl.pallas_call(
        functools.partial(kernel, sizes),
        out_shape=carried,
        in_specs=[pl.BlockSpec(memory_space=pl.ANY)] * 2,
        out_specs=(pl.BlockSpec(memory_space=pltpu.VMEM),) * len(carried),
        scratch_shapes=[
            pltpu.VMEM((planes + 2 * RADIUS, rows, columns), f32),
            pltpu.VMEM((blocks + 2, rows, columns), f32),
            pltpu.VMEM((blocks + 2,) + mask.shape[1:], jnp.int32),
            pltpu.VMEM((planes, rows, columns), f32),
            pltpu.VMEM((final, nx, rows, columns), f32),
            pltpu.VMEM((final, nx, 2 * SUBLANES, columns), f32),
            xs,
            dma((blocks,)),
            dma,
            dma((2,)),
            dma((2,)),
            dma((2, RADIUS)),
            dma((2, RADIUS)),
            dma((layers, nx)),
            dma((layers, nx)),
            dma((layers, 2)),
            dma((layers, 2)),
            dma((2, nx)),
            dma((2, nx)),
        ],
        compiler_params=pltpu.CompilerParams(
            collective_id=0, has_side_effects=True, vmem_limit_bytes=44 * 1024 * 1024
        ),
    )(density, mask)
    return pl.pallas_call(
        functools.partial(closing, sizes),
        out_shape=(shape((layers, rows, width), f32),) * 2,
        in_specs=[pl.BlockSpec(memory_space=pltpu.VMEM)] * len(carried),
        out_specs=(pl.BlockSpec(memory_space=pl.ANY),) * 2,
        scratch_shapes=[
            xs,
            pltpu.VMEM((rows, width), f32),
            pltpu.VMEM((rows, width), f32),
            dma((2, final)),
            dma((2, nx)),
        ],
        compiler_params=pltpu.CompilerParams(vmem_limit_bytes=16 * 1024 * 1024),
    )(*held)


def solution(mesh):
    sizes = (mesh.shape["gz"], mesh.shape["gx"], mesh.shape["gy"])
    placed = (P("gz", "gy", "gx"), P("gz", "gy", "gx"))
    return jax.shard_map(
        functools.partial(body, sizes),
        mesh=mesh,
        in_specs=placed,
        out_specs=(P(("gz", "gx"), "gy", None), P(("gz", "gx"), "gy", None)),
        check_vma=False,
    )
```

```python
import functools
import math

import jax
import jax.numpy as jnp
from jax import lax
from jax.experimental import pallas as pl
from jax.experimental.pallas import tpu as pltpu
from jax.sharding import PartitionSpec as P

RADIUS = 6
CELLS = 8
LANES = 128
SUBLANES = 8

sharpness = 8.0
threshold = 0.5
MESH = pl.DeviceIdType.MESH


def hat(rows, cols, offset):
    row = lax.broadcasted_iota(jnp.int32, (rows, cols), 0)
    col = lax.broadcasted_iota(jnp.int32, (rows, cols), 1)
    return jnp.maximum(RADIUS + 1 - jnp.abs(col + offset - row), 0).astype(jnp.float32)


def halves(values):
    high = values.astype(jnp.bfloat16)
    low = (values - high.astype(jnp.float32)).astype(jnp.bfloat16)
    return high, low


def projection(filtered):
    top = math.tanh(sharpness * threshold)
    bottom = top + math.tanh(sharpness * (1.0 - threshold))
    return (top + jnp.tanh(sharpness * (filtered - threshold))) * (1.0 / bottom)


def one_side(reach):
    return reach * (RADIUS + 1) - reach * (reach + 1) // 2


def dot(a, b):
    return jnp.dot(a, b, preferred_element_type=jnp.float32)


def x_filter(chunks, w_own, w_edge, xs, first):
    size, columns = chunks[0].shape
    high, low = zip(*[halves(chunk) for chunk in chunks])
    none = jnp.zeros((size, LANES), jnp.bfloat16)
    for c in range(len(chunks)):
        total = dot(high[c], w_own[...]) + dot(low[c], w_own[...])
        for part in (high, low):
            left = part[c - 1][:, columns - LANES :] if c > 0 else none
            right = part[c + 1][:, :LANES] if c < len(chunks) - 1 else none
            total = total + dot(jnp.concatenate([left, right], 1), w_edge[...])
        at = pl.ds(c * columns, columns)
        xs[pl.ds(first, size), at], xs[pl.ds(first + size, size), at] = halves(total)


def y_filter(xs, scale, scale_z, columns, put):
    rows, width = scale.shape
    own = hat(rows, rows, 0).astype(jnp.bfloat16)
    edge = jnp.concatenate([hat(rows, SUBLANES, -SUBLANES), hat(rows, SUBLANES, rows)], 1)
    edge = edge.astype(jnp.bfloat16)
    own = jnp.concatenate([own, own], 1)
    edge = jnp.concatenate([edge, edge], 1)
    for c in range(width // columns):
        at = pl.ds(c * columns, columns)
        summed = dot(own, xs[pl.ds(0, 2 * rows), at])
        summed = summed + dot(edge, xs[pl.ds(2 * rows, 4 * SUBLANES), at])
        put(at, summed * (scale[:, at] * scale_z))


def inverse_count(position, length):
    left = one_side(jnp.minimum(position, RADIUS))
    right = one_side(jnp.minimum(length - 1 - position, RADIUS))
    return 1.0 / (RADIUS + 1 + left + right).astype(jnp.float32)


def layer_of(k, layers):
    return jnp.where(lax.axis_index("gx") == 0, layers - 1 - k, k)


def scale_along_z(sizes, k, layers, columns):
    nz, nx, ny = sizes
    level = (lax.axis_index("gz") * nx + lax.axis_index("gx")) * layers + layer_of(k, layers)
    level = jnp.full((SUBLANES, columns), level, jnp.int32)
    return inverse_count(level, nz * nx * layers)[0:1]


def kernel(
    sizes,
    density,
    mask,
    fstage,
    pstage,
    lrecv,
    lyb,
    scale,
    w_own,
    w_edge,
    phys,
    codes,
    masks,
    zf,
    recv,
    yb,
    xs,
    load_sem,
    mask_sem,
    hmask_send,
    hmask_recv,
    halo_send,
    halo_recv,
    send_sem,
    recv_sem,
    y_send,
    y_recv,
    e_send,
    e_recv,
):
    nz, nx, ny = sizes
    planes, rows, columns = density.shape
    blocks = mask.shape[0]
    layers = planes // nx
    gz, gx, gy = lax.axis_index("gz"), lax.axis_index("gx"), lax.axis_index("gy")
    has_up, has_down = gz > 0, gz < nz - 1
    has_prev, has_next = gy > 0, gy < ny - 1

    def load(b):
        part = pl.ds(b * CELLS, CELLS)
        return pltpu.make_async_copy(
            density.at[part], phys.at[pl.ds(RADIUS + b * CELLS, CELLS)], load_sem.at[b]
        )

    mask_copy = pltpu.make_async_copy(mask, masks.at[pl.ds(1, blocks)], mask_sem)
    mask_copy.start()
    for b in range(blocks):
        load(b).start()

    barrier = pltpu.get_barrier_semaphore()

    def greet(**where):
        pl.semaphore_signal(barrier, inc=1, device_id=where, device_id_type=MESH)

    pl.when(has_up)(lambda: greet(gz=gz - 1))
    pl.when(has_down)(lambda: greet(gz=gz + 1))
    pl.when(has_prev)(lambda: greet(gy=gy - 1))
    pl.when(has_next)(lambda: greet(gy=gy + 1))
    for step in range(1, nx):
        greet(gx=lax.rem(gx + step, nx))

    def to_next(j):
        return pltpu.make_async_remote_copy(
            src_ref=density.at[planes - 1 - j],
            dst_ref=phys.at[RADIUS - 1 - j],
            send_sem=halo_send.at[0, j],
            recv_sem=halo_recv.at[0, j],
            device_id={"gz": gz + 1},
            device_id_type=MESH,
        )

    def to_previous(j):
        return pltpu.make_async_remote_copy(
            src_ref=density.at[j],
            dst_ref=phys.at[RADIUS + planes + j],
            send_sem=halo_send.at[1, j],
            recv_sem=halo_recv.at[1, j],
            device_id={"gz": gz - 1},
            device_id_type=MESH,
        )

    def mask_next():
        return pltpu.make_async_remote_copy(
            src_ref=mask.at[blocks - 1],
            dst_ref=masks.at[0],
            send_sem=hmask_send.at[0],
            recv_sem=hmask_recv.at[0],
            device_id={"gz": gz + 1},
            device_id_type=MESH,
        )

    def mask_previous():
        return pltpu.make_async_remote_copy(
            src_ref=mask.at[0],
            dst_ref=masks.at[blocks + 1],
            send_sem=hmask_send.at[1],
            recv_sem=hmask_recv.at[1],
            device_id={"gz": gz - 1},
            device_id_type=MESH,
        )

    def spread(b):
        small = masks[b].astype(jnp.float32).astype(jnp.bfloat16)
        mrows, mcols = small.shape
        r = lax.broadcasted_iota(jnp.int32, (rows, mrows), 0) // CELLS
        m = lax.broadcasted_iota(jnp.int32, (rows, mrows), 1)
        tall = dot(jnp.where(r == m, 1.0, 0.0).astype(jnp.bfloat16), small)
        c = lax.broadcasted_iota(jnp.int32, (mcols, columns), 1) // CELLS
        n = lax.broadcasted_iota(jnp.int32, (mcols, columns), 0)
        wide = jnp.where(c == n, 1.0, 0.0).astype(jnp.bfloat16)
        codes[b] = dot(tall.astype(jnp.bfloat16), wide)

    def apply_mask(row, b):
        code = codes[b]
        phys[row] = jnp.where(code < 0.5, 0.0, jnp.where(code < 1.5, 1.0, phys[row]))

    def piece(k, p, row):
        return pltpu.make_async_remote_copy(
            src_ref=zf.at[row],
            dst_ref=recv.at[k, gx],
            send_sem=send_sem.at[k, p],
            recv_sem=recv_sem.at[k, gx],
            device_id={"gx": p},
            device_id_type=MESH,
        )

    edges = (pl.ds(0, SUBLANES), pl.ds(rows - SUBLANES, SUBLANES))
    inside = pl.ds(SUBLANES, rows - 2 * SUBLANES)

    def edge_piece(side, p, row):
        return pltpu.make_async_remote_copy(
            src_ref=zf.at[row, edges[side]],
            dst_ref=lrecv.at[gx, edges[side]],
            send_sem=e_send.at[side, p],
            recv_sem=e_recv.at[side, gx],
            device_id={"gx": p},
            device_id_type=MESH,
        )

    def inner_piece(p, row):
        return pltpu.make_async_remote_copy(
            src_ref=zf.at[row, inside],
            dst_ref=lrecv.at[gx, inside],
            send_sem=send_sem.at[layers - 1, p],
            recv_sem=recv_sem.at[layers - 1, gx],
            device_id={"gx": p},
            device_id_type=MESH,
        )

    def row_of(k, p):
        return layers - 1 - k if p == 0 else p * layers + k

    def z_filter(row):
        part = rows // 4
        for i in range(4):
            at = pl.ds(i * part, part)
            run = phys[row + RADIUS, at]
            total = run
            for d in range(1, RADIUS + 1):
                run = run + (phys[row + RADIUS - d, at] + phys[row + RADIUS + d, at])
                total = total + run
            zf[row, at] = total

    def z_send(k, p):
        row = row_of(k, p)
        z_filter(row)

        @pl.when(gx != p)
        def _():
            piece(k, p, row).start()

        @pl.when(gx == p)
        def _():
            pltpu.make_async_copy(zf.at[row], recv.at[k, gx], recv_sem.at[k, gx]).start()

    def z_step(k, carry):
        for p in range(nx):
            z_send(k, p)
        return carry

    def mask_block(b):
        load(b).wait()

        def one(i, carry):
            apply_mask(RADIUS + b * CELLS + i, b + 1)
            return carry

        lax.fori_loop(0, CELLS, one, 0)

    mask_copy.wait()
    for b in range(blocks):
        spread(b + 1)
    ready = 0
    for p in range(nx):
        need = min(blocks, (row_of(0, p) + RADIUS) // CELLS + 1)
        for b in range(ready, need):
            mask_block(b)
        if p == 0:
            count = nx - 1
            for there in (has_up, has_down, has_prev, has_next):
                count = count + there.astype(jnp.int32)
            pl.semaphore_wait(barrier, count)
        ready = max(ready, need)
        z_send(0, p)
    for b in range(ready, blocks):
        mask_block(b)

    @pl.when(has_down)
    def _():
        mask_next().start()
        for j in range(RADIUS):
            to_next(j).start()

    @pl.when(has_up)
    def _():
        mask_previous().start()
        for j in range(RADIUS):
            to_previous(j).start()

    @pl.when(jnp.logical_not(has_up))
    def _():
        phys[pl.ds(0, RADIUS)] = jnp.zeros((RADIUS, rows, columns), jnp.float32)

    @pl.when(jnp.logical_not(has_down))
    def _():
        phys[pl.ds(RADIUS + planes, RADIUS)] = jnp.zeros((RADIUS, rows, columns), jnp.float32)

    @pl.when(jnp.logical_not(has_prev))
    def _():
        lyb[:, pl.ds(0, SUBLANES)] = jnp.zeros((nx, SUBLANES, columns), jnp.float32)
        yb[:, :, pl.ds(0, SUBLANES)] = jnp.zeros((layers - 1, nx, SUBLANES, columns), jnp.float32)

    @pl.when(jnp.logical_not(has_next))
    def _():
        lyb[:, pl.ds(SUBLANES, SUBLANES)] = jnp.zeros((nx, SUBLANES, columns), jnp.float32)
        yb[:, :, pl.ds(SUBLANES, SUBLANES)] = jnp.zeros((layers - 1, nx, SUBLANES, columns), jnp.float32)

    free = layers - RADIUS
    lax.fori_loop(1, free, z_step, 0)

    w_own[...] = hat(columns, columns, 0).astype(jnp.bfloat16)
    w_edge[pl.ds(0, LANES)] = hat(LANES, columns, LANES).astype(jnp.bfloat16)
    w_edge[pl.ds(LANES, LANES)] = hat(LANES, columns, -columns).astype(jnp.bfloat16)

    width = nx * columns
    scale_y = inverse_count(
        gy * rows + lax.broadcasted_iota(jnp.int32, (rows, LANES), 0), rows * ny
    )
    for c in range(0, width, LANES):
        lane = c + lax.broadcasted_iota(jnp.int32, (SUBLANES, LANES), 1)
        scale_x = inverse_count(lane, width)
        scale[:, pl.ds(c, LANES)] = scale_y * scale_x[0:1]

    @pl.when(has_up)
    def _():
        mask_previous().wait_send()
        pltpu.make_async_copy(mask.at[0], masks.at[0], hmask_recv.at[0]).wait()
        spread(0)

    @pl.when(has_down)
    def _():
        mask_next().wait_send()
        pltpu.make_async_copy(mask.at[0], masks.at[blocks + 1], hmask_recv.at[1]).wait()
        spread(blocks + 1)

    def take_halo(k):
        j = k - free

        @pl.when(has_up)
        def _():
            row = RADIUS - 1 - j
            pltpu.make_async_copy(density.at[0], phys.at[row], halo_recv.at[0, j]).wait()
            apply_mask(row, 0)

        @pl.when(has_down)
        def _():
            row = RADIUS + planes + j
            pltpu.make_async_copy(density.at[0], phys.at[row], halo_recv.at[1, j]).wait()
            apply_mask(row, blocks + 1)

    def halo_step(k, carry):
        take_halo(k)
        return z_step(k, carry)

    final = layers - 1
    lax.fori_loop(free, final, halo_step, 0)

    take_halo(final)
    for p in range(nx):
        row = row_of(final, p)
        z_filter(row)

        @pl.when(gx != p)
        def _():
            edge_piece(0, p, row).start()
            edge_piece(1, p, row).start()

        @pl.when(gx == p)
        def _():
            for side in range(2):
                pltpu.make_async_copy(
                    zf.at[row, edges[side]], lrecv.at[gx, edges[side]], e_recv.at[side, gx]
                ).start()
            pltpu.make_async_copy(
                zf.at[row, inside], lrecv.at[gx, inside], recv_sem.at[final, gx]
            ).start()

    mirror = nx - 1 - gx

    @pl.when(gx != mirror)
    def _():
        row = jnp.where(mirror == 0, layers - 1 - final, mirror * layers + final)
        inner_piece(mirror, row).start()

    for p in range(nx):

        @pl.when(jnp.logical_and(gx != p, mirror != p))
        def _():
            inner_piece(p, row_of(final, p)).start()

    def y_previous(k):
        return pltpu.make_async_remote_copy(
            src_ref=recv.at[k, :, pl.ds(0, SUBLANES)],
            dst_ref=yb.at[k, :, pl.ds(SUBLANES, SUBLANES)],
            send_sem=y_send.at[k, 0],
            recv_sem=y_recv.at[k, 1],
            device_id={"gy": gy - 1},
            device_id_type=MESH,
        )

    def y_next(k):
        return pltpu.make_async_remote_copy(
            src_ref=recv.at[k, :, pl.ds(rows - SUBLANES, SUBLANES)],
            dst_ref=yb.at[k, :, pl.ds(0, SUBLANES)],
            send_sem=y_send.at[k, 1],
            recv_sem=y_recv.at[k, 0],
            device_id={"gy": gy + 1},
            device_id_type=MESH,
        )

    def last_previous():
        return pltpu.make_async_remote_copy(
            src_ref=lrecv.at[:, pl.ds(0, SUBLANES)],
            dst_ref=lyb.at[:, pl.ds(SUBLANES, SUBLANES)],
            send_sem=y_send.at[final, 0],
            recv_sem=y_recv.at[final, 1],
            device_id={"gy": gy - 1},
            device_id_type=MESH,
        )

    def last_next():
        return pltpu.make_async_remote_copy(
            src_ref=lrecv.at[:, pl.ds(rows - SUBLANES, SUBLANES)],
            dst_ref=lyb.at[:, pl.ds(0, SUBLANES)],
            send_sem=y_send.at[final, 1],
            recv_sem=y_recv.at[final, 0],
            device_id={"gy": gy + 1},
            device_id_type=MESH,
        )

    def send_edges(k):
        pl.when(has_prev)(lambda: y_previous(k).start())
        pl.when(has_next)(lambda: y_next(k).start())

    def take_edges(k):
        @pl.when(has_prev)
        def _():
            y_previous(k).wait_send()
            part = yb.at[k, :, pl.ds(0, SUBLANES)]
            pltpu.make_async_copy(part, part, y_recv.at[k, 0]).wait()

        @pl.when(has_next)
        def _():
            y_next(k).wait_send()
            part = yb.at[k, :, pl.ds(SUBLANES, SUBLANES)]
            pltpu.make_async_copy(part, part, y_recv.at[k, 1]).wait()

    def take_step(k, carry):
        for c in range(nx):
            pltpu.make_async_copy(zf.at[0], recv.at[k, c], recv_sem.at[k, c]).wait()
        send_edges(k)
        x_filter([recv[k, c] for c in range(nx)], w_own, w_edge, xs, 0)
        take_edges(k)
        x_filter([yb[k, c] for c in range(nx)], w_own, w_edge, xs, 2 * rows)

        def put(at, value):
            fstage[k, :, at] = value
            pstage[k, :, at] = projection(value)

        y_filter(xs, scale, scale_along_z(sizes, k, layers, columns), columns, put)
        return carry

    lax.fori_loop(0, final, take_step, 0)

    for c in range(nx):
        for side in range(2):
            part = lrecv.at[c, edges[side]]
            pltpu.make_async_copy(part, part, e_recv.at[side, c]).wait()
    pl.when(has_prev)(lambda: last_previous().start())
    pl.when(has_next)(lambda: last_next().start())

    @pl.when(has_down)
    def _():
        for j in range(RADIUS):
            to_next(j).wait_send()

    @pl.when(has_up)
    def _():
        for j in range(RADIUS):
            to_previous(j).wait_send()

    def settle(k, carry):
        for p in range(nx):

            @pl.when(gx != p)
            def _():
                piece(k, p, 0).wait_send()

        return carry

    lax.fori_loop(0, final, settle, 0)
    for p in range(nx):

        @pl.when(gx != p)
        def _():
            edge_piece(0, p, 0).wait_send()
            edge_piece(1, p, 0).wait_send()
            inner_piece(p, 0).wait_send()

    @pl.when(has_prev)
    def _():
        last_previous().wait_send()
        part = lyb.at[:, pl.ds(0, SUBLANES)]
        pltpu.make_async_copy(part, part, y_recv.at[final, 0]).wait()

    @pl.when(has_next)
    def _():
        last_next().wait_send()
        part = lyb.at[:, pl.ds(SUBLANES, SUBLANES)]
        pltpu.make_async_copy(part, part, y_recv.at[final, 1]).wait()

    for c in range(nx):
        part = lrecv.at[c, inside]
        pltpu.make_async_copy(part, part, recv_sem.at[final, c]).wait()


def closing(sizes, fstage, pstage, lrecv, lyb, scale, w_own, w_edge, filt, proj, xs, flast, plast, sems, last_sems):
    final = fstage.shape[0]
    nx, rows, columns = lrecv.shape
    layers = final + 1

    def finished(k):
        at = layer_of(k, layers)
        return (
            pltpu.make_async_copy(fstage.at[k], filt.at[at], sems.at[0, k]),
            pltpu.make_async_copy(pstage.at[k], proj.at[at], sems.at[1, k]),
        )

    for k in range(final):
        for copy in finished(k):
            copy.start()
    x_filter([lrecv[c] for c in range(nx)], w_own, w_edge, xs, 0)
    x_filter([lyb[c] for c in range(nx)], w_own, w_edge, xs, 2 * rows)

    level = layer_of(final, layers)

    def ends(at):
        c = at.start // columns
        return (
            pltpu.make_async_copy(flast.at[:, at], filt.at[level, :, at], last_sems.at[0, c]),
            pltpu.make_async_copy(plast.at[:, at], proj.at[level, :, at], last_sems.at[1, c]),
        )

    def put(at, value):
        flast[:, at] = value
        first, second = ends(at)
        first.start()
        plast[:, at] = projection(value)
        second.start()

    y_filter(xs, scale, scale_along_z(sizes, final, layers, columns), columns, put)
    for k in range(final):
        for copy in finished(k):
            copy.wait()
    for c in range(nx):
        for copy in ends(pl.ds(c * columns, columns)):
            copy.wait()


def body(sizes, density, mask):
    planes, rows, columns = density.shape
    nz, nx, ny = sizes
    layers = planes // nx
    final = layers - 1
    blocks = mask.shape[0]
    width = nx * columns
    dma = pltpu.SemaphoreType.DMA
    f32, bf16 = jnp.float32, jnp.bfloat16
    shape = jax.ShapeDtypeStruct
    carried = (
        shape((final, rows, width), f32),
        shape((final, rows, width), f32),
        shape((nx, rows, columns), f32),
        shape((nx, 2 * SUBLANES, columns), f32),
        shape((rows, width), f32),
        shape((columns, columns), bf16),
        shape((2 * LANES, columns), bf16),
    )
    xs = pltpu.VMEM((2 * rows + 4 * SUBLANES, width), bf16)
    held = pl.pallas_call(
        functools.partial(kernel, sizes),
        out_shape=carried,
        in_specs=[pl.BlockSpec(memory_space=pl.ANY)] * 2,
        out_specs=(pl.BlockSpec(memory_space=pltpu.VMEM),) * len(carried),
        scratch_shapes=[
            pltpu.VMEM((planes + 2 * RADIUS, rows, columns), f32),
            pltpu.VMEM((blocks + 2, rows, columns), f32),
            pltpu.VMEM((blocks + 2,) + mask.shape[1:], jnp.int32),
            pltpu.VMEM((planes, rows, columns), f32),
            pltpu.VMEM((final, nx, rows, columns), f32),
            pltpu.VMEM((final, nx, 2 * SUBLANES, columns), f32),
            xs,
            dma((blocks,)),
            dma,
            dma((2,)),
            dma((2,)),
            dma((2, RADIUS)),
            dma((2, RADIUS)),
            dma((layers, nx)),
            dma((layers, nx)),
            dma((layers, 2)),
            dma((layers, 2)),
            dma((2, nx)),
            dma((2, nx)),
        ],
        compiler_params=pltpu.CompilerParams(
            collective_id=0, has_side_effects=True, vmem_limit_bytes=44 * 1024 * 1024
        ),
    )(density, mask)
    return pl.pallas_call(
        functools.partial(closing, sizes),
        out_shape=(shape((layers, rows, width), f32),) * 2,
        in_specs=[pl.BlockSpec(memory_space=pltpu.VMEM)] * len(carried),
        out_specs=(pl.BlockSpec(memory_space=pl.ANY),) * 2,
        scratch_shapes=[
            xs,
            pltpu.VMEM((rows, width), f32),
            pltpu.VMEM((rows, width), f32),
            dma((2, final)),
            dma((2, nx)),
        ],
        compiler_params=pltpu.CompilerParams(vmem_limit_bytes=16 * 1024 * 1024),
    )(*held)


def solution(mesh):
    sizes = (mesh.shape["gz"], mesh.shape["gx"], mesh.shape["gy"])
    placed = (P("gz", "gy", "gx"), P("gz", "gy", "gx"))
    return jax.shard_map(
        functools.partial(body, sizes),
        mesh=mesh,
        in_specs=placed,
        out_specs=(P(("gz", "gx"), "gy", None), P(("gz", "gx"), "gy", None)),
        check_vma=False,
    )
```

```python
import functools
import math

import jax
import jax.numpy as jnp
from jax import lax
from jax.experimental import pallas as pl
from jax.experimental.pallas import tpu as pltpu
from jax.sharding import PartitionSpec as P

RADIUS = 6
CELLS = 8
LANES = 128
SUBLANES = 8

sharpness = 8.0
threshold = 0.5
MESH = pl.DeviceIdType.MESH


def hat(rows, cols, offset):
    row = lax.broadcasted_iota(jnp.int32, (rows, cols), 0)
    col = lax.broadcasted_iota(jnp.int32, (rows, cols), 1)
    return jnp.maximum(RADIUS + 1 - jnp.abs(col + offset - row), 0).astype(jnp.float32)


def halves(values):
    high = values.astype(jnp.bfloat16)
    low = (values - high.astype(jnp.float32)).astype(jnp.bfloat16)
    return high, low


def projection(filtered):
    top = math.tanh(sharpness * threshold)
    bottom = top + math.tanh(sharpness * (1.0 - threshold))
    return (top + jnp.tanh(sharpness * (filtered - threshold))) * (1.0 / bottom)


def one_side(reach):
    return reach * (RADIUS + 1) - reach * (reach + 1) // 2


def dot(a, b):
    return jnp.dot(a, b, preferred_element_type=jnp.float32)


def x_filter(chunks, w_own, w_edge, xs, first):
    size, columns = chunks[0].shape
    high, low = zip(*[halves(chunk) for chunk in chunks])
    none = jnp.zeros((size, LANES), jnp.bfloat16)
    for c in range(len(chunks)):
        total = dot(high[c], w_own[...]) + dot(low[c], w_own[...])
        for part in (high, low):
            left = part[c - 1][:, columns - LANES :] if c > 0 else none
            right = part[c + 1][:, :LANES] if c < len(chunks) - 1 else none
            total = total + dot(jnp.concatenate([left, right], 1), w_edge[...])
        at = pl.ds(c * columns, columns)
        xs[pl.ds(first, size), at], xs[pl.ds(first + size, size), at] = halves(total)


def y_filter(xs, scale, scale_z, columns, put):
    rows, width = scale.shape
    own = hat(rows, rows, 0).astype(jnp.bfloat16)
    edge = jnp.concatenate([hat(rows, SUBLANES, -SUBLANES), hat(rows, SUBLANES, rows)], 1)
    edge = edge.astype(jnp.bfloat16)
    own = jnp.concatenate([own, own], 1)
    edge = jnp.concatenate([edge, edge], 1)
    for c in range(width // columns):
        at = pl.ds(c * columns, columns)
        summed = dot(own, xs[pl.ds(0, 2 * rows), at])
        summed = summed + dot(edge, xs[pl.ds(2 * rows, 4 * SUBLANES), at])
        put(at, summed * (scale[:, at] * scale_z))


def inverse_count(position, length):
    left = one_side(jnp.minimum(position, RADIUS))
    right = one_side(jnp.minimum(length - 1 - position, RADIUS))
    return 1.0 / (RADIUS + 1 + left + right).astype(jnp.float32)


def layer_of(k, layers):
    return jnp.where(lax.axis_index("gx") == 0, layers - 1 - k, k)


def scale_along_z(sizes, k, layers, columns):
    nz, nx, ny = sizes
    level = (lax.axis_index("gz") * nx + lax.axis_index("gx")) * layers + layer_of(k, layers)
    level = jnp.full((SUBLANES, columns), level, jnp.int32)
    return inverse_count(level, nz * nx * layers)[0:1]


def kernel(
    sizes,
    density,
    mask,
    fstage,
    pstage,
    lrecv,
    lyb,
    scale,
    w_own,
    w_edge,
    phys,
    codes,
    masks,
    zf,
    recv,
    yb,
    xs,
    load_sem,
    mask_sem,
    hmask_send,
    hmask_recv,
    halo_send,
    halo_recv,
    send_sem,
    recv_sem,
    y_send,
    y_recv,
    e_send,
    e_recv,
):
    nz, nx, ny = sizes
    planes, rows, columns = density.shape
    blocks = mask.shape[0]
    layers = planes // nx
    gz, gx, gy = lax.axis_index("gz"), lax.axis_index("gx"), lax.axis_index("gy")
    has_up, has_down = gz > 0, gz < nz - 1
    has_prev, has_next = gy > 0, gy < ny - 1

    def load(b):
        part = pl.ds(b * CELLS, CELLS)
        return pltpu.make_async_copy(
            density.at[part], phys.at[pl.ds(RADIUS + b * CELLS, CELLS)], load_sem.at[b]
        )

    mask_copy = pltpu.make_async_copy(mask, masks.at[pl.ds(1, blocks)], mask_sem)
    mask_copy.start()
    for b in range(blocks):
        load(b).start()

    barrier = pltpu.get_barrier_semaphore()

    def greet(**where):
        pl.semaphore_signal(barrier, inc=1, device_id=where, device_id_type=MESH)

    pl.when(has_up)(lambda: greet(gz=gz - 1))
    pl.when(has_down)(lambda: greet(gz=gz + 1))
    pl.when(has_prev)(lambda: greet(gy=gy - 1))
    pl.when(has_next)(lambda: greet(gy=gy + 1))
    for step in range(1, nx):
        greet(gx=lax.rem(gx + step, nx))

    def to_next(j):
        return pltpu.make_async_remote_copy(
            src_ref=density.at[planes - 1 - j],
            dst_ref=phys.at[RADIUS - 1 - j],
            send_sem=halo_send.at[0, j],
            recv_sem=halo_recv.at[0, j],
            device_id={"gz": gz + 1},
            device_id_type=MESH,
        )

    def to_previous(j):
        return pltpu.make_async_remote_copy(
            src_ref=density.at[j],
            dst_ref=phys.at[RADIUS + planes + j],
            send_sem=halo_send.at[1, j],
            recv_sem=halo_recv.at[1, j],
            device_id={"gz": gz - 1},
            device_id_type=MESH,
        )

    def mask_next():
        return pltpu.make_async_remote_copy(
            src_ref=mask.at[blocks - 1],
            dst_ref=masks.at[0],
            send_sem=hmask_send.at[0],
            recv_sem=hmask_recv.at[0],
            device_id={"gz": gz + 1},
            device_id_type=MESH,
        )

    def mask_previous():
        return pltpu.make_async_remote_copy(
            src_ref=mask.at[0],
            dst_ref=masks.at[blocks + 1],
            send_sem=hmask_send.at[1],
            recv_sem=hmask_recv.at[1],
            device_id={"gz": gz - 1},
            device_id_type=MESH,
        )

    def spread(b):
        small = masks[b].astype(jnp.float32).astype(jnp.bfloat16)
        mrows, mcols = small.shape
        r = lax.broadcasted_iota(jnp.int32, (rows, mrows), 0) // CELLS
        m = lax.broadcasted_iota(jnp.int32, (rows, mrows), 1)
        tall = dot(jnp.where(r == m, 1.0, 0.0).astype(jnp.bfloat16), small)
        c = lax.broadcasted_iota(jnp.int32, (mcols, columns), 1) // CELLS
        n = lax.broadcasted_iota(jnp.int32, (mcols, columns), 0)
        wide = jnp.where(c == n, 1.0, 0.0).astype(jnp.bfloat16)
        codes[b] = dot(tall.astype(jnp.bfloat16), wide)

    def apply_mask(row, b):
        code = codes[b]
        phys[row] = jnp.where(code < 0.5, 0.0, jnp.where(code < 1.5, 1.0, phys[row]))

    def piece(k, p, row):
        return pltpu.make_async_remote_copy(
            src_ref=zf.at[row],
            dst_ref=recv.at[k, gx],
            send_sem=send_sem.at[k, p],
            recv_sem=recv_sem.at[k, gx],
            device_id={"gx": p},
            device_id_type=MESH,
        )

    edges = (pl.ds(0, SUBLANES), pl.ds(rows - SUBLANES, SUBLANES))
    inside = pl.ds(SUBLANES, rows - 2 * SUBLANES)

    def edge_piece(side, p, row):
        return pltpu.make_async_remote_copy(
            src_ref=zf.at[row, edges[side]],
            dst_ref=lrecv.at[gx, edges[side]],
            send_sem=e_send.at[side, p],
            recv_sem=e_recv.at[side, gx],
            device_id={"gx": p},
            device_id_type=MESH,
        )

    def inner_piece(p, row):
        return pltpu.make_async_remote_copy(
            src_ref=zf.at[row, inside],
            dst_ref=lrecv.at[gx, inside],
            send_sem=send_sem.at[layers - 1, p],
            recv_sem=recv_sem.at[layers - 1, gx],
            device_id={"gx": p},
            device_id_type=MESH,
        )

    def row_of(k, p):
        return layers - 1 - k if p == 0 else p * layers + k

    def z_filter(row):
        part = rows // 4
        for i in range(4):
            at = pl.ds(i * part, part)
            run = phys[row + RADIUS, at]
            total = run
            for d in range(1, RADIUS + 1):
                run = run + (phys[row + RADIUS - d, at] + phys[row + RADIUS + d, at])
                total = total + run
            zf[row, at] = total

    def z_send(k, p):
        row = row_of(k, p)
        z_filter(row)

        @pl.when(gx != p)
        def _():
            piece(k, p, row).start()

        @pl.when(gx == p)
        def _():
            pltpu.make_async_copy(zf.at[row], recv.at[k, gx], recv_sem.at[k, gx]).start()

    def z_step(k, carry):
        for p in range(nx):
            z_send(k, p)
        return carry

    def mask_block(b):
        spread(b + 1)
        load(b).wait()

        def one(i, carry):
            apply_mask(RADIUS + b * CELLS + i, b + 1)
            return carry

        lax.fori_loop(0, CELLS, one, 0)

    mask_copy.wait()
    ready = 0
    for p in range(nx):
        need = min(blocks, (row_of(0, p) + RADIUS) // CELLS + 1)
        for b in range(ready, need):
            mask_block(b)
        if p == 0:
            count = nx - 1
            for there in (has_up, has_down, has_prev, has_next):
                count = count + there.astype(jnp.int32)
            pl.semaphore_wait(barrier, count)
        ready = max(ready, need)
        z_send(0, p)
    for b in range(ready, blocks):
        mask_block(b)

    @pl.when(has_down)
    def _():
        mask_next().start()
        for j in range(RADIUS):
            to_next(j).start()

    @pl.when(has_up)
    def _():
        mask_previous().start()
        for j in range(RADIUS):
            to_previous(j).start()

    @pl.when(jnp.logical_not(has_up))
    def _():
        phys[pl.ds(0, RADIUS)] = jnp.zeros((RADIUS, rows, columns), jnp.float32)

    @pl.when(jnp.logical_not(has_down))
    def _():
        phys[pl.ds(RADIUS + planes, RADIUS)] = jnp.zeros((RADIUS, rows, columns), jnp.float32)

    @pl.when(jnp.logical_not(has_prev))
    def _():
        lyb[:, pl.ds(0, SUBLANES)] = jnp.zeros((nx, SUBLANES, columns), jnp.float32)
        yb[:, :, pl.ds(0, SUBLANES)] = jnp.zeros((layers - 1, nx, SUBLANES, columns), jnp.float32)

    @pl.when(jnp.logical_not(has_next))
    def _():
        lyb[:, pl.ds(SUBLANES, SUBLANES)] = jnp.zeros((nx, SUBLANES, columns), jnp.float32)
        yb[:, :, pl.ds(SUBLANES, SUBLANES)] = jnp.zeros((layers - 1, nx, SUBLANES, columns), jnp.float32)

    free = layers - RADIUS
    lax.fori_loop(1, free, z_step, 0)

    w_own[...] = hat(columns, columns, 0).astype(jnp.bfloat16)
    w_edge[pl.ds(0, LANES)] = hat(LANES, columns, LANES).astype(jnp.bfloat16)
    w_edge[pl.ds(LANES, LANES)] = hat(LANES, columns, -columns).astype(jnp.bfloat16)

    width = nx * columns
    scale_y = inverse_count(
        gy * rows + lax.broadcasted_iota(jnp.int32, (rows, LANES), 0), rows * ny
    )
    for c in range(0, width, LANES):
        lane = c + lax.broadcasted_iota(jnp.int32, (SUBLANES, LANES), 1)
        scale_x = inverse_count(lane, width)
        scale[:, pl.ds(c, LANES)] = scale_y * scale_x[0:1]

    @pl.when(has_up)
    def _():
        mask_previous().wait_send()
        pltpu.make_async_copy(mask.at[0], masks.at[0], hmask_recv.at[0]).wait()
        spread(0)

    @pl.when(has_down)
    def _():
        mask_next().wait_send()
        pltpu.make_async_copy(mask.at[0], masks.at[blocks + 1], hmask_recv.at[1]).wait()
        spread(blocks + 1)

    def take_halo(k):
        j = k - free

        @pl.when(has_up)
        def _():
            row = RADIUS - 1 - j
            pltpu.make_async_copy(density.at[0], phys.at[row], halo_recv.at[0, j]).wait()
            apply_mask(row, 0)

        @pl.when(has_down)
        def _():
            row = RADIUS + planes + j
            pltpu.make_async_copy(density.at[0], phys.at[row], halo_recv.at[1, j]).wait()
            apply_mask(row, blocks + 1)

    def halo_step(k, carry):
        take_halo(k)
        return z_step(k, carry)

    final = layers - 1
    lax.fori_loop(free, final, halo_step, 0)

    take_halo(final)
    for p in range(nx):
        row = row_of(final, p)
        z_filter(row)

        @pl.when(gx != p)
        def _():
            edge_piece(0, p, row).start()
            edge_piece(1, p, row).start()

        @pl.when(gx == p)
        def _():
            for side in range(2):
                pltpu.make_async_copy(
                    zf.at[row, edges[side]], lrecv.at[gx, edges[side]], e_recv.at[side, gx]
                ).start()
            pltpu.make_async_copy(
                zf.at[row, inside], lrecv.at[gx, inside], recv_sem.at[final, gx]
            ).start()

    for p in range(nx):

        @pl.when(gx != p)
        def _():
            inner_piece(p, row_of(final, p)).start()

    def y_previous(k):
        return pltpu.make_async_remote_copy(
            src_ref=recv.at[k, :, pl.ds(0, SUBLANES)],
            dst_ref=yb.at[k, :, pl.ds(SUBLANES, SUBLANES)],
            send_sem=y_send.at[k, 0],
            recv_sem=y_recv.at[k, 1],
            device_id={"gy": gy - 1},
            device_id_type=MESH,
        )

    def y_next(k):
        return pltpu.make_async_remote_copy(
            src_ref=recv.at[k, :, pl.ds(rows - SUBLANES, SUBLANES)],
            dst_ref=yb.at[k, :, pl.ds(0, SUBLANES)],
            send_sem=y_send.at[k, 1],
            recv_sem=y_recv.at[k, 0],
            device_id={"gy": gy + 1},
            device_id_type=MESH,
        )

    def last_previous():
        return pltpu.make_async_remote_copy(
            src_ref=lrecv.at[:, pl.ds(0, SUBLANES)],
            dst_ref=lyb.at[:, pl.ds(SUBLANES, SUBLANES)],
            send_sem=y_send.at[final, 0],
            recv_sem=y_recv.at[final, 1],
            device_id={"gy": gy - 1},
            device_id_type=MESH,
        )

    def last_next():
        return pltpu.make_async_remote_copy(
            src_ref=lrecv.at[:, pl.ds(rows - SUBLANES, SUBLANES)],
            dst_ref=lyb.at[:, pl.ds(0, SUBLANES)],
            send_sem=y_send.at[final, 1],
            recv_sem=y_recv.at[final, 0],
            device_id={"gy": gy + 1},
            device_id_type=MESH,
        )

    def send_edges(k):
        pl.when(has_prev)(lambda: y_previous(k).start())
        pl.when(has_next)(lambda: y_next(k).start())

    def take_edges(k):
        @pl.when(has_prev)
        def _():
            y_previous(k).wait_send()
            part = yb.at[k, :, pl.ds(0, SUBLANES)]
            pltpu.make_async_copy(part, part, y_recv.at[k, 0]).wait()

        @pl.when(has_next)
        def _():
            y_next(k).wait_send()
            part = yb.at[k, :, pl.ds(SUBLANES, SUBLANES)]
            pltpu.make_async_copy(part, part, y_recv.at[k, 1]).wait()

    def take_step(k, carry):
        for c in range(nx):
            pltpu.make_async_copy(zf.at[0], recv.at[k, c], recv_sem.at[k, c]).wait()
        send_edges(k)
        x_filter([recv[k, c] for c in range(nx)], w_own, w_edge, xs, 0)
        take_edges(k)
        x_filter([yb[k, c] for c in range(nx)], w_own, w_edge, xs, 2 * rows)

        def put(at, value):
            fstage[k, :, at] = value
            pstage[k, :, at] = projection(value)

        y_filter(xs, scale, scale_along_z(sizes, k, layers, columns), columns, put)
        return carry

    lax.fori_loop(0, final, take_step, 0)

    for c in range(nx):
        for side in range(2):
            part = lrecv.at[c, edges[side]]
            pltpu.make_async_copy(part, part, e_recv.at[side, c]).wait()
    pl.when(has_prev)(lambda: last_previous().start())
    pl.when(has_next)(lambda: last_next().start())

    @pl.when(has_down)
    def _():
        for j in range(RADIUS):
            to_next(j).wait_send()

    @pl.when(has_up)
    def _():
        for j in range(RADIUS):
            to_previous(j).wait_send()

    def settle(k, carry):
        for p in range(nx):

            @pl.when(gx != p)
            def _():
                piece(k, p, 0).wait_send()

        return carry

    lax.fori_loop(0, final, settle, 0)
    for p in range(nx):

        @pl.when(gx != p)
        def _():
            edge_piece(0, p, 0).wait_send()
            edge_piece(1, p, 0).wait_send()
            inner_piece(p, 0).wait_send()

    @pl.when(has_prev)
    def _():
        last_previous().wait_send()
        part = lyb.at[:, pl.ds(0, SUBLANES)]
        pltpu.make_async_copy(part, part, y_recv.at[final, 0]).wait()

    @pl.when(has_next)
    def _():
        last_next().wait_send()
        part = lyb.at[:, pl.ds(SUBLANES, SUBLANES)]
        pltpu.make_async_copy(part, part, y_recv.at[final, 1]).wait()

    for c in range(nx):
        part = lrecv.at[c, inside]
        pltpu.make_async_copy(part, part, recv_sem.at[final, c]).wait()


def closing(sizes, fstage, pstage, lrecv, lyb, scale, w_own, w_edge, filt, proj, xs, flast, plast, sems, last_sems):
    final = fstage.shape[0]
    nx, rows, columns = lrecv.shape
    layers = final + 1

    def finished(k):
        at = layer_of(k, layers)
        return (
            pltpu.make_async_copy(fstage.at[k], filt.at[at], sems.at[0, k]),
            pltpu.make_async_copy(pstage.at[k], proj.at[at], sems.at[1, k]),
        )

    for k in range(final):
        for copy in finished(k):
            copy.start()
    x_filter([lrecv[c] for c in range(nx)], w_own, w_edge, xs, 0)
    x_filter([lyb[c] for c in range(nx)], w_own, w_edge, xs, 2 * rows)

    def put(at, value):
        flast[:, at] = value
        plast[:, at] = projection(value)

    y_filter(xs, scale, scale_along_z(sizes, final, layers, columns), columns, put)
    at = layer_of(final, layers)
    ends = (
        pltpu.make_async_copy(flast, filt.at[at], last_sems.at[0]),
        pltpu.make_async_copy(plast, proj.at[at], last_sems.at[1]),
    )
    for copy in ends:
        copy.start()
    for k in range(final):
        for copy in finished(k):
            copy.wait()
    for copy in ends:
        copy.wait()


def body(sizes, density, mask):
    planes, rows, columns = density.shape
    nz, nx, ny = sizes
    layers = planes // nx
    final = layers - 1
    blocks = mask.shape[0]
    width = nx * columns
    dma = pltpu.SemaphoreType.DMA
    f32, bf16 = jnp.float32, jnp.bfloat16
    shape = jax.ShapeDtypeStruct
    carried = (
        shape((final, rows, width), f32),
        shape((final, rows, width), f32),
        shape((nx, rows, columns), f32),
        shape((nx, 2 * SUBLANES, columns), f32),
        shape((rows, width), f32),
        shape((columns, columns), bf16),
        shape((2 * LANES, columns), bf16),
    )
    xs = pltpu.VMEM((2 * rows + 4 * SUBLANES, width), bf16)
    held = pl.pallas_call(
        functools.partial(kernel, sizes),
        out_shape=carried,
        in_specs=[pl.BlockSpec(memory_space=pl.ANY)] * 2,
        out_specs=(pl.BlockSpec(memory_space=pltpu.VMEM),) * len(carried),
        scratch_shapes=[
            pltpu.VMEM((planes + 2 * RADIUS, rows, columns), f32),
            pltpu.VMEM((blocks + 2, rows, columns), f32),
            pltpu.VMEM((blocks + 2,) + mask.shape[1:], jnp.int32),
            pltpu.VMEM((planes, rows, columns), f32),
            pltpu.VMEM((final, nx, rows, columns), f32),
            pltpu.VMEM((final, nx, 2 * SUBLANES, columns), f32),
            xs,
            dma((blocks,)),
            dma,
            dma((2,)),
            dma((2,)),
            dma((2, RADIUS)),
            dma((2, RADIUS)),
            dma((layers, nx)),
            dma((layers, nx)),
            dma((layers, 2)),
            dma((layers, 2)),
            dma((2, nx)),
            dma((2, nx)),
        ],
        compiler_params=pltpu.CompilerParams(
            collective_id=0, has_side_effects=True, vmem_limit_bytes=44 * 1024 * 1024
        ),
    )(density, jnp.minimum(mask, 2))
    return pl.pallas_call(
        functools.partial(closing, sizes),
        out_shape=(shape((layers, rows, width), f32),) * 2,
        in_specs=[pl.BlockSpec(memory_space=pltpu.VMEM)] * len(carried),
        out_specs=(pl.BlockSpec(memory_space=pl.ANY),) * 2,
        scratch_shapes=[
            xs,
            pltpu.VMEM((rows, width), f32),
            pltpu.VMEM((rows, width), f32),
            dma((2, final)),
            dma((2,)),
        ],
        compiler_params=pltpu.CompilerParams(vmem_limit_bytes=16 * 1024 * 1024),
    )(*held)


def solution(mesh):
    sizes = (mesh.shape["gz"], mesh.shape["gx"], mesh.shape["gy"])
    placed = (P("gz", "gy", "gx"), P("gz", "gy", "gx"))
    return jax.shard_map(
        functools.partial(body, sizes),
        mesh=mesh,
        in_specs=placed,
        out_specs=(P(("gz", "gx"), "gy", None), P(("gz", "gx"), "gy", None)),
        check_vma=False,
    )
```
